32 devices in a mesh: tgt: 4 (over y, core), src: 8 (over z, x).
Axes of the slice: x: 2, y: 2, z: 4, core: 2. Of those that a mesh axis runs over, the one named last changes fastest.
Arguments:
- mobility: bfloat16 [3, 3, 4, 8, 64, 2048], P(None, None, None, 'src', None, 'tgt'), may hold values from -0.078125 to 0.078125
- right_side: float32 [3, 2048, 512], P(None, ('tgt', 'src')), may hold values from -6 to 6
- precond: float32 [96, 6144], P(None, ('tgt', 'src')), may hold values from -0.5 to 2.5
Outputs:
- solution: float32 [3, 2048, 512], P(None, ('tgt', 'src'))
- arnoldi: float32 [3, 2, 512], replicated
The draws below stay inside these ranges and needn't reach their ends.
All inputs are finite; a program needn't handle non-finite values.
Results may differ from the reference program's by a relative error of at most 0.0012.
Values may be sent and summed in bfloat16 or wider, within the bound.
No kernel may reach another device: no remote copies, remote signals or barrier semaphores. Data moves between devices by JAX's collectives and lax.ppermute only.
A program may use at most 64 MiB of HBM per device.

```python
import jax
import jax.numpy as jnp
from jax import lax

FIBER_NODES = 32
CASES = 512
NODE_DEV = 64
NODES = 2048
N_TGT = 4
N_SRC = 8


def draw_precond(key, part):
    fibers = NODES // FIBER_NODES
    width = 3 * FIBER_NODES
    key_one, key_two = jax.random.split(jax.random.fold_in(key, 23), 2)
    diagonal = jnp.exp(jax.random.uniform(key_one, (fibers, width), jnp.float32, jnp.log(0.5), jnp.log(2.0)))
    spread = jnp.clip(jax.random.normal(key_two, (fibers, width, width), jnp.float32), -6.0, 6.0) * (0.4 / jnp.sqrt(float(width)))
    blocks = spread + diagonal[:, :, None] * jnp.eye(width, dtype=jnp.float32)[None]
    return blocks.transpose(1, 0, 2).reshape(width, fibers * width).astype(jnp.float32)


def shard_levels(key, dims, cuts, least, high):
    factor_of = 1.0
    for dim, blocks in cuts:
        heights = jax.random.uniform(jax.random.fold_in(jax.random.fold_in(key, 6), dim), (blocks,), jnp.float32, least / len(cuts), high / len(cuts))
        factor_of = factor_of * jnp.repeat(jnp.exp(heights), dims[dim] // blocks).reshape((-1,) + (1,) * (len(dims) - 1 - dim))
    return factor_of


def noise(rng, dims, scale, limit, cuts=(), held_as=jnp.bfloat16):
    values = jax.random.normal(rng, dims, jnp.float32) * scale
    if len(cuts) > 0:
        values = shard_levels(rng, dims, cuts, -0.22, 0.18) * values
    return jnp.clip(values, min=-limit, max=limit).astype(held_as)


def setup_inputs(seed: int = 0) -> dict:
    keys = jax.random.split(jax.random.key(seed), 4)
    mobility = noise(keys[0], (3, 3, N_TGT, N_SRC, NODE_DEV, NODES), (3 * NODES) ** -0.5, 0.078125, ((3, 8), (5, 4)))
    right_side = noise(keys[1], (3, NODES, CASES), 1.0, 6.0, ((1, 32),), jnp.float32)
    precond = draw_precond(jax.random.fold_in(keys[3], 71), 0)
    return dict(mobility=mobility, right_side=right_side, precond=precond)


def couple(mobility, vector):
    matrix = mobility.reshape(3, 3, NODES, NODES)
    rounded = vector.astype(jnp.bfloat16)
    parts = []
    for comp in range(3):
        total = jnp.zeros((NODES, vector.shape[2]), jnp.float32)
        for source in range(3):
            total = total + lax.dot_general(matrix[source, comp], rounded[source], (((0,), (0,)), ((), ())), preferred_element_type=jnp.float32)
        parts.append(total)
    return jnp.stack(parts)

def apply_blocks(blocks, vector):
    width = 3 * FIBER_NODES
    fibers = blocks.shape[1] // width
    case_count = vector.shape[2]
    tiles = blocks.reshape(width, fibers, width)
    arranged = vector.reshape(3, fibers, FIBER_NODES, case_count).transpose(1, 0, 2, 3).reshape(fibers, width, case_count)
    result = jnp.einsum('afb,fbr->far', tiles, arranged, precision=lax.Precision.HIGHEST)
    return result.reshape(fibers, 3, FIBER_NODES, case_count).transpose(1, 0, 2, 3).reshape(3, fibers * FIBER_NODES, case_count)

def least_squares(beta, h_one_one, h_two_one, h_one_two, h_two_two, h_three_two):
    rho_one = jnp.sqrt(h_one_one * h_one_one + h_two_one * h_two_one)
    cos_one = h_one_one / rho_one
    sin_one = h_two_one / rho_one
    g_one = cos_one * beta
    g_two = -sin_one * beta
    top = cos_one * h_one_two + sin_one * h_two_two
    low = cos_one * h_two_two - sin_one * h_one_two
    rho_two = jnp.sqrt(low * low + h_three_two * h_three_two)
    cos_two = low / rho_two
    sin_two = h_three_two / rho_two
    y_two = cos_two * g_two / rho_two
    y_one = (g_one - top * y_two) / rho_one
    return (y_one, y_two, jnp.abs(sin_two * g_two))

def inner(first, second):
    return lax.optimization_barrier(jnp.sum(first * second, axis=(0, 1)))

def reference(mobility, right_side, precond):

    def operate(vector):
        return vector + couple(mobility, vector)
    initial = apply_blocks(precond, right_side)
    beta = jnp.sqrt(inner(initial, initial) + 1e-06)
    basis_one = initial / beta[None, None, :]
    work = apply_blocks(precond, operate(basis_one))
    h_one_one = inner(basis_one, work)
    work = work - h_one_one[None, None, :] * basis_one
    h_two_one = jnp.sqrt(inner(work, work) + 1e-06)
    basis_two = work / h_two_one[None, None, :]
    other = apply_blocks(precond, operate(basis_two))
    h_one_two = inner(basis_one, other)
    h_two_two = inner(basis_two, other)
    other = other - h_one_two[None, None, :] * basis_one - h_two_two[None, None, :] * basis_two
    h_three_two = jnp.sqrt(inner(other, other) + 1e-06)
    y_one, y_two, estimate = least_squares(beta, h_one_one, h_two_one, h_one_two, h_two_two, h_three_two)
    solution = y_one[None, None, :] * basis_one + y_two[None, None, :] * basis_two
    arnoldi = jnp.stack([jnp.stack([h_one_one, h_one_two]), jnp.stack([h_two_one, h_two_two]), jnp.stack([estimate, h_three_two])])
    return (solution, arnoldi)
```

```python
import jax
import jax.numpy as jnp
from jax import lax
from jax.sharding import PartitionSpec as P

FIBER_NODES = 32
PIECES = 3
PAD_ROWS = 16


def apply_blocks(blocks, vector):
    width = 3 * FIBER_NODES
    fibers = blocks.shape[1] // width
    case_count = vector.shape[2]
    tiles = blocks.reshape(width, fibers, width)
    arranged = (
        vector.reshape(3, fibers, FIBER_NODES, case_count)
        .transpose(1, 0, 2, 3)
        .reshape(fibers, width, case_count)
    )
    result = jnp.einsum("afb,fbr->far", tiles, arranged, precision=lax.Precision.HIGHEST)
    return (
        result.reshape(fibers, 3, FIBER_NODES, case_count)
        .transpose(1, 0, 2, 3)
        .reshape(3, fibers * FIBER_NODES, case_count)
    )


def least_squares(beta, h_one_one, h_two_one, h_one_two, h_two_two, h_three_two):
    rho_one = jnp.sqrt(h_one_one * h_one_one + h_two_one * h_two_one)
    cos_one = h_one_one / rho_one
    sin_one = h_two_one / rho_one
    g_one = cos_one * beta
    g_two = -sin_one * beta
    top = cos_one * h_one_two + sin_one * h_two_two
    low = cos_one * h_two_two - sin_one * h_one_two
    rho_two = jnp.sqrt(low * low + h_three_two * h_three_two)
    cos_two = low / rho_two
    sin_two = h_three_two / rho_two
    y_two = cos_two * g_two / rho_two
    y_one = (g_one - top * y_two) / rho_one
    return (y_one, y_two, jnp.abs(sin_two * g_two))


def inner(first, second):
    return jnp.sum(first * second, axis=(0, 1))


def split_rows(rows):
    pieces = []
    rest = rows
    for _ in range(PIECES):
        head = lax.reduce_precision(rest, 8, 7)
        pieces.append(head)
        rest = rest - head
    stacked = jnp.concatenate(pieces)
    stacked = jnp.pad(stacked, ((0, PAD_ROWS - stacked.shape[0]), (0, 0)))
    return stacked.astype(jnp.bfloat16)


def join_rows(stacked, count):
    wide = stacked[:, : PIECES * count].astype(jnp.float32)
    total = jnp.sum(wide, axis=0).reshape(PIECES, count, -1)
    return jnp.sum(total, axis=0)


def local(mobility, right_side, precond):
    row_count = mobility.shape[5]
    sources = mobility.shape[2]
    node_dev = mobility.shape[4]
    targets = row_count // node_dev
    cases = right_side.shape[2]
    local_tile = mobility.reshape(3, 3, sources * node_dev, row_count)

    height = 3 * node_dev

    def operate(vector, rows, terms):
        count = rows.shape[0]
        heads = []
        rest = vector.reshape(height, cases)
        for _ in range(terms):
            head = lax.reduce_precision(rest, 8, 7)
            heads.append(head.astype(jnp.bfloat16))
            rest = rest - head
        got = lax.all_gather(jnp.concatenate(heads + [split_rows(rows)]), "tgt")
        partial_value = 0.0
        for term in range(terms):
            piece = got[:, term * height : (term + 1) * height].reshape(sources, 3, node_dev, cases)
            piece = piece.transpose(1, 0, 2, 3).reshape(3, sources * node_dev, cases)
            partial_value = partial_value + lax.dot_general(
                local_tile, piece, (((0, 2), (0, 1)), ((), ())), preferred_element_type=jnp.float32
            )
        outgoing = (
            partial_value.astype(jnp.bfloat16)
            .reshape(3, targets, node_dev, cases)
            .transpose(1, 0, 2, 3)
            .reshape(targets, height, cases)
        )
        extra = split_rows(join_rows(got[:, terms * height :], count))
        outgoing = jnp.concatenate(
            [outgoing, jnp.broadcast_to(extra, (targets,) + extra.shape)], axis=1
        )
        arrived = lax.all_to_all(outgoing, "src", 0, 0)
        own_share = jnp.sum(arrived[:, : height].astype(jnp.float32), axis=0)
        total = join_rows(arrived[:, height :], count)
        return vector + own_share.reshape(3, node_dev, cases), total

    def total_of(rows):
        first = jnp.sum(lax.all_to_all(jnp.broadcast_to(rows, (sources,) + rows.shape), "tgt", 0, 0), axis=0)
        return jnp.sum(lax.all_to_all(jnp.broadcast_to(first, (targets,) + rows.shape), "src", 0, 0), axis=0)

    start = apply_blocks(precond, right_side)
    moved, sums = operate(start, inner(start, start)[None], 2)
    beta = jnp.sqrt(sums[0] + 1e-06)
    basis_one = start / beta[None, None, :]
    work = apply_blocks(precond, moved) / beta[None, None, :]
    moved, sums = operate(work, inner(basis_one, work)[None], 1)
    h_one_one = sums[0]
    other = apply_blocks(precond, moved) - h_one_one[None, None, :] * work
    work = work - h_one_one[None, None, :] * basis_one
    gram = total_of(
        jnp.stack(
            [
                inner(work, work),
                inner(basis_one, other),
                inner(work, other),
                inner(other, other),
                inner(basis_one, work),
                inner(basis_one, basis_one),
                jnp.zeros((cases,), jnp.float32),
                jnp.zeros((cases,), jnp.float32),
            ]
        )
    )
    work_work, one_other, work_other, other_other, one_work, one_one = (gram[k] for k in range(6))
    h_two_one = jnp.sqrt(work_work + 1e-06)
    basis_two = work / h_two_one[None, None, :]
    h_one_two = one_other / h_two_one
    h_two_two = work_other / (h_two_one * h_two_one)
    two_two = work_work / (h_two_one * h_two_one)
    one_two = one_work / h_two_one
    rest = (
        other_other / (h_two_one * h_two_one)
        - h_one_two * h_one_two * (2.0 - one_one)
        - h_two_two * h_two_two * (2.0 - two_two)
        + 2.0 * h_one_two * h_two_two * one_two
    )
    h_three_two = jnp.sqrt(jnp.maximum(rest, 0.0) + 1e-06)
    y_one, y_two, estimate = least_squares(
        beta, h_one_one, h_two_one, h_one_two, h_two_two, h_three_two
    )
    solution = y_one[None, None, :] * basis_one + y_two[None, None, :] * basis_two
    arnoldi = jnp.stack(
        [
            jnp.stack([h_one_one, h_one_two]),
            jnp.stack([h_two_one, h_two_two]),
            jnp.stack([estimate, h_three_two]),
        ]
    )
    return (solution, arnoldi)


def solution(mesh):
    placed = (
        P(None, None, None, "src", None, "tgt"),
        P(None, ("tgt", "src"), None),
        P(None, ("tgt", "src")),
    )
    return jax.shard_map(
        local,
        mesh=mesh,
        in_specs=placed,
        out_specs=(P(None, ("tgt", "src"), None), P()),
        check_vma=False,
    )
```

```python
import jax
import jax.numpy as jnp
from jax import lax
from jax.sharding import Mesh, PartitionSpec as P

FIBER_NODES = 32
PIECES = 3
PAD_ROWS = 8


def apply_blocks(blocks, vector):
    width = 3 * FIBER_NODES
    fibers = blocks.shape[1] // width
    case_count = vector.shape[2]
    tiles = blocks.reshape(width, fibers, width)
    arranged = (
        vector.reshape(3, fibers, FIBER_NODES, case_count)
        .transpose(1, 0, 2, 3)
        .reshape(fibers, width, case_count)
    )
    result = jnp.einsum("afb,fbr->far", tiles, arranged, precision=lax.Precision.HIGHEST)
    return (
        result.reshape(fibers, 3, FIBER_NODES, case_count)
        .transpose(1, 0, 2, 3)
        .reshape(3, fibers * FIBER_NODES, case_count)
    )


def least_squares(beta, h_one_one, h_two_one, h_one_two, h_two_two, h_three_two):
    rho_one = jnp.sqrt(h_one_one * h_one_one + h_two_one * h_two_one)
    cos_one = h_one_one / rho_one
    sin_one = h_two_one / rho_one
    g_one = cos_one * beta
    g_two = -sin_one * beta
    top = cos_one * h_one_two + sin_one * h_two_two
    low = cos_one * h_two_two - sin_one * h_one_two
    rho_two = jnp.sqrt(low * low + h_three_two * h_three_two)
    cos_two = low / rho_two
    sin_two = h_three_two / rho_two
    y_two = cos_two * g_two / rho_two
    y_one = (g_one - top * y_two) / rho_one
    return (y_one, y_two, jnp.abs(sin_two * g_two))


def inner(first, second):
    return jnp.sum(first * second, axis=(0, 1))


def split_rows(rows):
    pieces = []
    rest = rows
    for _ in range(PIECES):
        head = lax.reduce_precision(rest, 8, 7)
        pieces.append(head)
        rest = rest - head
    stacked = jnp.concatenate(pieces)
    stacked = jnp.pad(stacked, ((0, PAD_ROWS - stacked.shape[0]), (0, 0)))
    return stacked.astype(jnp.bfloat16)


def join_rows(stacked, count):
    wide = stacked[:, : PIECES * count].astype(jnp.float32)
    total = jnp.sum(wide, axis=0).reshape(PIECES, count, -1)
    return jnp.sum(total, axis=0)


def local(mobility, right_side, precond):
    row_count = mobility.shape[5]
    sources = mobility.shape[2]
    node_dev = mobility.shape[4]
    targets = row_count // node_dev
    cases = right_side.shape[2]
    local_tile = mobility.reshape(3, 3, sources * node_dev, row_count)

    height = 3 * node_dev

    def operate(vector, rows, terms):
        count = rows.shape[0]
        heads = []
        rest = vector.reshape(height, cases)
        for _ in range(terms):
            head = lax.reduce_precision(rest, 8, 7)
            heads.append(head.astype(jnp.bfloat16))
            rest = rest - head
        near = lax.all_gather(jnp.concatenate(heads + [split_rows(rows)]), "row")
        cuts = [term * height for term in range(terms)] + [near.shape[1]]
        got = [
            lax.all_gather(near[:, first:last], "core", axis=1)
            for first, last in zip(cuts[:-1], cuts[1:])
        ]
        got = [part.reshape((sources,) + part.shape[2:]) for part in got]
        partial_value = 0.0
        for term in range(terms):
            piece = got[term][:, :height].reshape(sources, 3, node_dev, cases)
            piece = piece.transpose(1, 0, 2, 3).reshape(3, sources * node_dev, cases)
            partial_value = partial_value + lax.dot_general(
                local_tile, piece, (((0, 2), (0, 1)), ((), ())), preferred_element_type=jnp.float32
            )
        outgoing = (
            partial_value.astype(jnp.bfloat16)
            .reshape(3, targets, node_dev, cases)
            .transpose(1, 0, 2, 3)
            .reshape(targets, height, cases)
        )
        extra = split_rows(join_rows(got[-1][:, height:], count))
        outgoing = jnp.concatenate(
            [outgoing, jnp.broadcast_to(extra, (targets,) + extra.shape)], axis=1
        )
        outgoing = outgoing.reshape(2, targets // 2, height + PAD_ROWS, cases)
        arrived = lax.all_to_all(outgoing, "near", 1, 1)
        summed = jnp.sum(arrived[:, :, :height].astype(jnp.float32), axis=1)
        sums = jnp.stack([join_rows(arrived[half, :, height:], count) for half in range(2)])
        side = lax.axis_index("half")
        keep = jnp.where(side == 0, summed[0], summed[1])
        give = jnp.where(side == 0, summed[1], summed[0])
        give = jnp.concatenate([give.astype(jnp.bfloat16), split_rows(sums[0])])
        taken = lax.ppermute(give, "half", [(0, 1), (1, 0)])
        own_share = keep + taken[:height].astype(jnp.float32)
        total = sums[0] + join_rows(taken[None, height:], count)
        return vector + own_share.reshape(3, node_dev, cases), total

    def total_of(rows):
        first = jnp.sum(lax.all_to_all(jnp.broadcast_to(rows, (sources,) + rows.shape), ("row", "core"), 0, 0), axis=0)
        return jnp.sum(lax.all_to_all(jnp.broadcast_to(first, (targets,) + rows.shape), ("half", "near"), 0, 0), axis=0)

    start = apply_blocks(precond, right_side)
    moved, sums = operate(start, inner(start, start)[None], 2)
    beta = jnp.sqrt(sums[0] + 1e-06)
    basis_one = start / beta[None, None, :]
    work = apply_blocks(precond, moved) / beta[None, None, :]
    moved, sums = operate(work, inner(basis_one, work)[None], 1)
    h_one_one = sums[0]
    other = apply_blocks(precond, moved) - h_one_one[None, None, :] * work
    work = work - h_one_one[None, None, :] * basis_one
    gram = total_of(
        jnp.stack(
            [
                inner(work, work),
                inner(basis_one, other),
                inner(work, other),
                inner(other, other),
                inner(basis_one, work),
                inner(basis_one, basis_one),
                jnp.zeros((cases,), jnp.float32),
                jnp.zeros((cases,), jnp.float32),
            ]
        )
    )
    work_work, one_other, work_other, other_other, one_work, one_one = (gram[k] for k in range(6))
    h_two_one = jnp.sqrt(work_work + 1e-06)
    basis_two = work / h_two_one[None, None, :]
    h_one_two = one_other / h_two_one
    h_two_two = work_other / (h_two_one * h_two_one)
    two_two = work_work / (h_two_one * h_two_one)
    one_two = one_work / h_two_one
    rest = (
        other_other / (h_two_one * h_two_one)
        - h_one_two * h_one_two * (2.0 - one_one)
        - h_two_two * h_two_two * (2.0 - two_two)
        + 2.0 * h_one_two * h_two_two * one_two
    )
    h_three_two = jnp.sqrt(jnp.maximum(rest, 0.0) + 1e-06)
    y_one, y_two, estimate = least_squares(
        beta, h_one_one, h_two_one, h_one_two, h_two_two, h_three_two
    )
    solution = y_one[None, None, :] * basis_one + y_two[None, None, :] * basis_two
    arnoldi = jnp.stack(
        [
            jnp.stack([h_one_one, h_one_two]),
            jnp.stack([h_two_one, h_two_two]),
            jnp.stack([estimate, h_three_two]),
        ]
    )
    return (solution, arnoldi)


def solution(mesh):
    count_tgt, count_src = mesh.shape["tgt"], mesh.shape["src"]
    grid = mesh.devices.reshape(count_tgt // 2, 2, 2, count_src // 2)
    fine = Mesh(grid, ("row", "core", "half", "near"))
    tgt = ("row", "core")
    src = ("half", "near")
    placed = (
        P(None, None, None, src, None, tgt),
        P(None, tgt + src, None),
        P(None, tgt + src),
    )
    return jax.shard_map(
        local,
        mesh=fine,
        in_specs=placed,
        out_specs=(P(None, tgt + src, None), P()),
        check_vma=False,
    )
```

```python
import jax
import jax.numpy as jnp
from jax import lax
from jax.sharding import Mesh, PartitionSpec as P

FIBER_NODES = 32
PIECES = 3
EXTRA = 8
SWAP = [(0, 1), (1, 0)]
TINY = 1e-06


def apply_blocks(blocks, vector):
    width = 3 * FIBER_NODES
    fibers = blocks.shape[1] // width
    case_count = vector.shape[2]
    tiles = blocks.reshape(width, fibers, width)
    arranged = (
        vector.reshape(3, fibers, FIBER_NODES, case_count)
        .transpose(1, 0, 2, 3)
        .reshape(fibers, width, case_count)
    )
    result = jnp.einsum("afb,fbr->far", tiles, arranged, precision=lax.Precision.HIGHEST)
    return (
        result.reshape(fibers, 3, FIBER_NODES, case_count)
        .transpose(1, 0, 2, 3)
        .reshape(3, fibers * FIBER_NODES, case_count)
    )


def least_squares(beta, h_one_one, h_two_one, h_one_two, h_two_two, h_three_two):
    rho_one = jnp.sqrt(h_one_one * h_one_one + h_two_one * h_two_one)
    cos_one = h_one_one / rho_one
    sin_one = h_two_one / rho_one
    g_one = cos_one * beta
    g_two = -sin_one * beta
    top = cos_one * h_one_two + sin_one * h_two_two
    low = cos_one * h_two_two - sin_one * h_one_two
    rho_two = jnp.sqrt(low * low + h_three_two * h_three_two)
    cos_two = low / rho_two
    sin_two = h_three_two / rho_two
    y_two = cos_two * g_two / rho_two
    y_one = (g_one - top * y_two) / rho_one
    return (y_one, y_two, jnp.abs(sin_two * g_two))


def inner(first, second):
    return jnp.sum(first * second, axis=(0, 1))


def pad_rows(rows):
    return jnp.pad(rows, ((0, EXTRA - rows.shape[0]), (0, 0)))


class Sums:
    dtype = jnp.bfloat16

    def __init__(self, rows):
        self.rows = rows

    def pack(self, body):
        pieces = []
        rest = self.rows
        for _ in range(PIECES):
            head = lax.reduce_precision(rest, 8, 7)
            pieces.append(head)
            rest = rest - head
        return body.astype(self.dtype), pad_rows(jnp.concatenate(pieces)).astype(self.dtype)

    def unpack(self, body, rows):
        count = self.rows.shape[0]
        wide = rows[: PIECES * count].astype(jnp.float32).reshape(PIECES, count, -1)
        return body.astype(jnp.float32), jnp.sum(wide, axis=0)

    def merge(self, other):
        return Sums(self.rows + other)

    def columns(self, first, last):
        return Sums(self.rows[:, first:last])


class Scale:
    dtype = jnp.float16

    def __init__(self, size):
        factors = []
        scale = jnp.ones_like(size)
        rest = size
        for _ in range(PIECES):
            factor = lax.reduce_precision(jnp.clip(rest, 2.0**-13, 2.0**15), 5, 10)
            factors.append(factor)
            scale = scale * factor
            rest = rest / factor
        self.factors = jnp.stack(factors)
        self.scale = scale

    def pack(self, body):
        scaled = body * (1.0 / self.scale)
        return scaled.astype(self.dtype), pad_rows(self.factors).astype(self.dtype)

    def unpack(self, body, rows):
        wide = rows[:PIECES].astype(jnp.float32)
        scale = wide[0] * wide[1] * wide[2]
        return body.astype(jnp.float32) * scale, scale

    def merge(self, other):
        return Scale(jnp.maximum(self.scale, other))

    def columns(self, first, last):
        return Scale(self.scale[first:last])


def pick(array, index, axis):
    return jnp.where(
        index == 0,
        lax.index_in_dim(array, 0, axis, False),
        lax.index_in_dim(array, 1, axis, False),
    )


def halve(array, note, names, name):
    axis = 1 + names.index(name)
    side = lax.axis_index(name)
    keep = pick(array, side, axis)
    body, rows = note.pack(pick(array, 1 - side, axis))
    sent = jnp.concatenate([body.reshape(-1, body.shape[-1]), rows])
    got = lax.ppermute(sent, name, SWAP)
    value, other = note.unpack(got[:-EXTRA].reshape(keep.shape), got[-EXTRA:])
    return keep + value, note.merge(other), [n for n in names if n != name]


def exchange(array, note, names):
    cases = array.shape[-1]
    half = cases // 2
    lower = names[1:]
    colours = [
        (array[..., :half], note.columns(0, half), names),
        (array[..., half:], note.columns(half, cases), names),
    ]
    for first, second in zip(reversed(lower), lower):
        colours = [halve(*colours[0], first), halve(*colours[1], second)]
    parts = [colour[0] for colour in colours]
    array = jnp.concatenate(parts, axis=-1)
    if isinstance(note, Sums):
        note = Sums(jnp.concatenate([colour[1].rows for colour in colours], axis=-1))
    else:
        note = Scale(jnp.concatenate([colour[1].scale for colour in colours], axis=-1))
    array, note, _ = halve(array, note, names[:1], names[0])
    return array, note


def build(bits):
    def local(mobility, right_side, precond):
        row_count = mobility.shape[5]
        sources = mobility.shape[2]
        node_dev = mobility.shape[4]
        cases = right_side.shape[2]
        height = 3 * node_dev
        local_tile = mobility.reshape(3, 3, sources * node_dev, row_count)

        def gather(vector, note):
            body, rows = note.pack(vector.reshape(height, cases))
            got = lax.all_gather(jnp.concatenate([body, rows]), ("row", "core"))
            return got[:, :height], got[:, height:]

        def arrange(got):
            piece = got.reshape(sources, 3, node_dev, cases).transpose(1, 0, 2, 3)
            return piece.reshape(3, sources * node_dev, cases)

        def couple(piece):
            return lax.dot_general(
                local_tile, piece, (((0, 2), (0, 1)), ((), ())), preferred_element_type=jnp.float32
            )

        def chunks(partial_value):
            return partial_value.reshape((3,) + (2,) * len(bits) + (node_dev, cases))

        start = apply_blocks(precond, right_side)
        note = Scale(jnp.max(jnp.abs(start), axis=(0, 1)))
        got, rows = gather(start, note)
        pairs = [note.unpack(got[k], rows[k]) for k in range(sources)]
        value = arrange(jnp.stack([pair[0] for pair in pairs]))
        head = lax.reduce_precision(value, 8, 7)
        tail = value - head
        partial_value = couple(head.astype(jnp.bfloat16)) + couple(tail.astype(jnp.bfloat16))
        size = jnp.max(jnp.stack([pair[1] for pair in pairs]), axis=0)
        share, _ = exchange(chunks(partial_value), Scale(size), bits)
        work = apply_blocks(precond, start + share)

        note = Sums(jnp.stack([inner(start, start), inner(start, work)]))
        got, rows = gather(work, note)
        total = sum(note.unpack(got[k], rows[k])[1] for k in range(sources))
        share, note = exchange(chunks(couple(arrange(got))), Sums(total), bits)
        start_start, start_work = note.rows[0], note.rows[1]
        square = start_start + TINY
        beta = jnp.sqrt(square)
        h_one_one = start_work / square
        other = apply_blocks(precond, work + share) - h_one_one[None, None, :] * work
        work = work - h_one_one[None, None, :] * start

        gram = jnp.stack(
            [inner(work, work), inner(start, other), inner(work, other), inner(other, other)]
        )
        flat = gram.reshape(-1, 128)
        flat = flat + lax.ppermute(flat, "core", SWAP)
        members = sources // 2 * 2 ** len(bits)
        flat = lax.all_to_all(
            jnp.broadcast_to(flat, (members,) + flat.shape), ("row",) + tuple(bits), 0, 0
        )
        work_work, start_other, work_other, other_other = jnp.sum(flat, axis=0).reshape(4, cases)

        norm = work_work / square
        h_two_one = jnp.sqrt(norm + TINY)
        length = beta * h_two_one
        h_one_two = start_other / (beta * length)
        h_two_two = work_other / (length * length)
        loss_one = TINY / square
        loss_two = TINY / (h_two_one * h_two_one)
        one_two = h_one_one * loss_one / h_two_one
        rest = (
            other_other / (length * length)
            - h_one_two * h_one_two * (1.0 + loss_one)
            - h_two_two * h_two_two * (1.0 + loss_two)
            + 2.0 * h_one_two * h_two_two * one_two
        )
        h_three_two = jnp.sqrt(jnp.maximum(rest, 0.0) + TINY)
        y_one, y_two, estimate = least_squares(
            beta, h_one_one, h_two_one, h_one_two, h_two_two, h_three_two
        )
        solution = (y_one / beta)[None, None, :] * start + (y_two / length)[None, None, :] * work
        arnoldi = jnp.stack(
            [
                jnp.stack([h_one_one, h_one_two]),
                jnp.stack([h_two_one, h_two_two]),
                jnp.stack([estimate, h_three_two]),
            ]
        )
        return (solution, arnoldi)

    return local


def solution(mesh):
    count_tgt, count_src = mesh.shape["tgt"], mesh.shape["src"]
    depth = count_src.bit_length() - 1
    bits = ["bit%d" % k for k in reversed(range(depth))]
    tgt = ("row", "core")
    src = tuple(bits)
    grid = mesh.devices.reshape((count_tgt // 2, 2) + (2,) * depth)
    placed = (
        P(None, None, None, src, None, tgt),
        P(None, tgt + src, None),
        P(None, tgt + src),
    )
    return jax.shard_map(
        build(bits),
        mesh=Mesh(grid, tgt + src),
        in_specs=placed,
        out_specs=(P(None, tgt + src, None), P()),
        check_vma=False,
    )
```

```python
import functools

import jax
import jax.numpy as jnp
from jax import lax
from jax.experimental import pallas as pl
from jax.experimental.pallas import tpu as pltpu
from jax.sharding import Mesh, PartitionSpec as P

FIBER_NODES = 32
PIECES = 3
EXTRA = 16
NOTE = 8
SWAP = [(0, 1), (1, 0)]
TINY = 1e-06
F32 = jnp.float32
BF16 = jnp.bfloat16


def least_squares(beta, h_one_one, h_two_one, h_one_two, h_two_two, h_three_two):
    rho_one = jnp.sqrt(h_one_one * h_one_one + h_two_one * h_two_one)
    cos_one = h_one_one / rho_one
    sin_one = h_two_one / rho_one
    g_one = cos_one * beta
    g_two = -sin_one * beta
    top = cos_one * h_one_two + sin_one * h_two_two
    low = cos_one * h_two_two - sin_one * h_one_two
    rho_two = jnp.sqrt(low * low + h_three_two * h_three_two)
    cos_two = low / rho_two
    sin_two = h_three_two / rho_two
    y_two = cos_two * g_two / rho_two
    y_one = (g_one - top * y_two) / rho_one
    return (y_one, y_two, jnp.abs(sin_two * g_two))


def stack_rows(rows, count):
    blank = jnp.zeros_like(rows[0])
    return jnp.concatenate(list(rows) + [blank] * (count - len(rows)), axis=0)


class Scale:
    sent = F32

    def __init__(self, size):
        factors = []
        scale = jnp.ones_like(size)
        rest = size
        for _ in range(PIECES):
            factor = jnp.clip(rest, 2.0**-13, 2.0**15).astype(BF16).astype(F32)
            factors.append(factor)
            scale = scale * factor
            rest = rest / factor
        self.scale = scale
        self.inverse = 1.0 / scale
        self.packed = stack_rows(factors, EXTRA)

    def pack(self, body):
        return body * self.inverse

    @staticmethod
    def read(rows):
        return rows[0:1] * rows[1:2] * rows[2:3]

    @staticmethod
    def unpack(body, other):
        return body * other

    @classmethod
    def load(cls, note):
        return cls(note[0:1, :])

    def merge(self, other):
        return Scale(jnp.maximum(self.scale, other))

    def rows(self):
        return stack_rows([self.scale], NOTE)


class Sums:
    sent = BF16

    def __init__(self, total):
        pieces = []
        rest = total
        for _ in range(PIECES):
            piece = rest.astype(BF16).astype(F32)
            pieces.append(piece)
            rest = rest - piece
        self.total = total
        self.packed = stack_rows(pieces, EXTRA).astype(BF16) if total.shape[0] == 1 else stack_rows(
            [piece[k : k + 1] for piece in pieces for k in range(2)], EXTRA
        ).astype(BF16)

    def pack(self, body):
        return body.astype(BF16)

    @staticmethod
    def read(rows):
        wide = rows.astype(F32)
        return wide[0:2] + wide[2:4] + wide[4:6]

    @staticmethod
    def unpack(body, other):
        return body.astype(F32)

    @classmethod
    def load(cls, note):
        return cls(note[0:2, :])

    def merge(self, other):
        return Sums(self.total + other)

    def rows(self):
        return stack_rows([self.total[0:1], self.total[1:2]], NOTE)


def insert(slot, place, side):
    low = slot & ((1 << place) - 1)
    return ((slot >> place) << (place + 1)) + (side << place) + low


def blocks_times(precond, value):
    width = 3 * FIBER_NODES
    fibers = precond.shape[1] // width
    nodes = fibers * FIBER_NODES
    results = []
    for fiber in range(fibers):
        parts = []
        for comp in range(3):
            first = comp * nodes + fiber * FIBER_NODES
            parts.append(value[first : first + FIBER_NODES])
        column = jnp.concatenate(parts, axis=0)
        blank = jnp.zeros_like(column)
        tall = [column if k == fiber else blank for k in range(fibers)]
        results.append(
            jnp.dot(
                precond,
                jnp.concatenate(tall, axis=0),
                precision=lax.Precision.HIGHEST,
                preferred_element_type=F32,
            )
        )
    parts = []
    for comp in range(3):
        for fiber in range(fibers):
            parts.append(results[fiber][comp * FIBER_NODES : (comp + 1) * FIBER_NODES])
    return jnp.concatenate(parts, axis=0)


def row_sum(first, second):
    return jnp.sum(first * second, axis=0, keepdims=True)


def first_body(right_ref, precond_ref, start_ref, sent_ref):
    height = start_ref.shape[0]
    start = blocks_times(precond_ref[...], right_ref[...])
    start_ref[...] = start
    note = Scale(jnp.max(jnp.abs(start), axis=0, keepdims=True))
    sent_ref[0:height] = note.pack(start)
    sent_ref[height:] = note.packed


def couple_body(kind, places, sides_ref, tile_ref, got_ref, *refs):
    sends, keeps, note_ref, work_ref = refs[0:2], refs[2:4], refs[4], refs[5]
    sources = got_ref.shape[0]
    height = got_ref.shape[1] - EXTRA
    nodes = height // 3
    cases = got_ref.shape[2]
    half = cases // 2
    targets = tile_ref.shape[3] // nodes
    others = [kind.read(got_ref[k, height:]) for k in range(sources)]
    blocks = []
    for comp in range(3):
        for k in range(sources):
            block = got_ref[k, comp * nodes : (comp + 1) * nodes]
            if kind is Scale:
                block = block * others[k]
            blocks.append(block)
    value = jnp.concatenate(blocks, axis=0)
    terms = [value.astype(BF16)]
    if kind is Scale:
        note = Scale(functools.reduce(jnp.maximum, others))
        terms.append((value - terms[0].astype(F32)).astype(BF16))
    else:
        note = Sums(functools.reduce(jnp.add, others))
    note_ref[...] = note.rows()
    for comp in range(3):
        left = tile_ref[:, comp].reshape(value.shape[0], targets * nodes)
        total = 0.0
        for term in terms:
            total = total + lax.dot_general(
                left, term, (((0,), (0,)), ((), ())), preferred_element_type=F32
            )
        work_ref[comp] = total
    for colour in range(2):
        first = colour * half
        columns = slice(first, first + half)
        side = sides_ref[colour]
        inner_note = type(note).load(note_ref[:, columns])
        for slot in range(targets // 2):
            give = insert(slot, places[colour], 1 - side) * nodes
            keep = insert(slot, places[colour], side) * nodes
            for comp in range(3):
                row = slot * height + comp * nodes
                value = work_ref[comp, pl.ds(pl.multiple_of(give, nodes), nodes), columns]
                sends[colour][row : row + nodes] = inner_note.pack(value)
                value = work_ref[comp, pl.ds(pl.multiple_of(keep, nodes), nodes), columns]
                keeps[colour][row : row + nodes] = value
        sends[colour][targets // 2 * height :] = inner_note.packed


def merge_body(kind, places, joined, height, sides_ref, note_ref, *refs):
    kept, got, outs, next_ref = refs[0:2], refs[2:4], refs[4:-1], refs[-1]
    half = kept[0].shape[1]
    slots = kept[0].shape[0] // height
    for colour in range(2):
        columns = slice(colour * half, (colour + 1) * half)
        side = sides_ref[colour]
        other = kind.read(got[colour][slots * height :])
        note = kind.load(note_ref[:, columns]).merge(other)
        next_ref[:, columns] = note.rows()
        for slot in range(slots // 2):
            rows = slice(slot * height, (slot + 1) * height)
            give = pl.ds(pl.multiple_of(insert(slot, places[colour], 1 - side) * height, height), height)
            keep = pl.ds(pl.multiple_of(insert(slot, places[colour], side) * height, height), height)
            given = note.pack(kept[colour][give] + kind.unpack(got[colour][give], other))
            held = kept[colour][keep] + kind.unpack(got[colour][keep], other)
            if joined:
                outs[0][rows, columns] = given
                outs[1][rows, columns] = held
            else:
                outs[colour][rows] = given
                outs[2 + colour][rows] = held
        if joined:
            outs[0][slots // 2 * height :, columns] = note.packed
        else:
            outs[colour][slots // 2 * height :] = note.packed


def second_body(kept_ref, got_ref, start_ref, precond_ref, work_ref, sent_ref):
    height = start_ref.shape[0]
    other = Scale.read(got_ref[height:])
    start = start_ref[...]
    moved = start + (kept_ref[...] + Scale.unpack(got_ref[0:height], other))
    work = blocks_times(precond_ref[...], moved)
    work_ref[...] = work
    note = Sums(jnp.concatenate([row_sum(start, start), row_sum(start, work)], axis=0))
    sent_ref[0:height] = note.pack(work)
    sent_ref[height:] = note.packed


def third_body(kept_ref, got_ref, note_ref, start_ref, work_ref, precond_ref, side_ref, gram_ref, next_ref):
    height = start_ref.shape[0]
    note = Sums.load(note_ref[...]).merge(Sums.read(got_ref[height:]))
    next_ref[...] = note.rows()
    start = start_ref[...]
    work = work_ref[...]
    moved = work + (kept_ref[...] + got_ref[0:height].astype(F32))
    h_one_one = note.total[1:2] / (note.total[0:1] + TINY)
    other = blocks_times(precond_ref[...], moved) - h_one_one * work
    side = work - h_one_one * start
    side_ref[...] = side
    pairs = [(side, side), (start, other), (side, other), (other, other)]
    rows = [row_sum(*pair) for pair in pairs]
    width = gram_ref.shape[1]
    count = rows[0].shape[1] // width
    parts = [row[:, k * width : (k + 1) * width] for row in rows for k in range(count)]
    gram_ref[...] = jnp.concatenate(parts, axis=0)


def last_body(flat_ref, note_ref, start_ref, side_ref, solution_ref, arnoldi_ref):
    total = jnp.sum(flat_ref[...], axis=0)
    count = total.shape[0] // 4
    gram = [
        jnp.concatenate([total[k * count + q : k * count + q + 1] for q in range(count)], axis=1)
        for k in range(4)
    ]
    side_side, start_other, side_other, other_other = gram
    square = note_ref[0:1, :] + TINY
    beta = jnp.sqrt(square)
    h_one_one = note_ref[1:2, :] / square
    h_two_one = jnp.sqrt(side_side / square + TINY)
    length = beta * h_two_one
    h_one_two = start_other / (beta * length)
    h_two_two = side_other / (length * length)
    loss_one = TINY / square
    loss_two = TINY / (h_two_one * h_two_one)
    one_two = h_one_one * loss_one / h_two_one
    rest = (
        other_other / (length * length)
        - h_one_two * h_one_two * (1.0 + loss_one)
        - h_two_two * h_two_two * (1.0 + loss_two)
        + 2.0 * h_one_two * h_two_two * one_two
    )
    h_three_two = jnp.sqrt(jnp.maximum(rest, 0.0) + TINY)
    y_one, y_two, estimate = least_squares(
        beta, h_one_one, h_two_one, h_one_two, h_two_two, h_three_two
    )
    solution_ref[...] = (y_one / beta) * start_ref[...] + (y_two / length) * side_ref[...]
    rows = [h_one_one, h_one_two, h_two_one, h_two_two, estimate, h_three_two]
    arnoldi_ref[...] = jnp.concatenate(rows, axis=0)


def call(body, shapes, *args, scalars=0, scratch=()):
    spec = pl.BlockSpec(memory_space=pltpu.VMEM)
    small = pl.BlockSpec(memory_space=pltpu.SMEM)
    return pl.pallas_call(
        body,
        out_shape=[jax.ShapeDtypeStruct(shape, dtype) for shape, dtype in shapes],
        in_specs=[small] * scalars + [spec] * (len(args) - scalars),
        out_specs=[spec] * len(shapes),
        scratch_shapes=list(scratch),
        compiler_params=pltpu.CompilerParams(vmem_limit_bytes=56 * 1024 * 1024),
    )(*args)


def travel(array, kind, move):
    if kind is Scale:
        return move(array.astype(jnp.float16)).astype(F32)
    return move(array)


def build(bits):
    lower = bits[1:]
    orders = (list(reversed(lower)), list(lower))

    def local(mobility, right_side, precond):
        row_count = mobility.shape[5]
        sources = mobility.shape[2]
        node_dev = mobility.shape[4]
        cases = right_side.shape[2]
        height = 3 * node_dev
        half = cases // 2
        tile = mobility.reshape(3, 3, sources * node_dev, row_count)
        right = right_side.reshape(height, cases)

        def sides(names):
            return jnp.stack([lax.axis_index(name).astype(jnp.int32) for name in names])

        def gather(sent, kind):
            return travel(sent, kind, lambda a: lax.all_gather(a, ("row", "core")))

        def exchange(got, kind):
            left = [list(bits), list(bits)]
            slots = row_count // node_dev
            for step in range(len(lower) + 1):
                joined = step == len(lower)
                names = [bits[0]] * 2 if joined else [orders[0][step], orders[1][step]]
                places = [len(left[k]) - 1 - left[k].index(names[k]) for k in range(2)]
                slots = slots // 2
                tall = slots * height
                note = ((NOTE, cases), F32)
                if step == 0:
                    shapes = [((tall + EXTRA, half), kind.sent)] * 2 + [((tall, half), F32)] * 2
                    outs = call(
                        functools.partial(couple_body, kind, places),
                        shapes + [note],
                        sides(names),
                        tile,
                        got,
                        scalars=1,
                        scratch=[pltpu.VMEM((3, row_count, cases), F32)],
                    )
                else:
                    shapes = [((tall + EXTRA, half), kind.sent)] * 2 + [((tall, half), F32)] * 2
                    if joined:
                        shapes = [((tall + EXTRA, cases), kind.sent), ((tall, cases), F32)]
                    outs = call(
                        functools.partial(merge_body, kind, places, joined, height),
                        shapes + [note],
                        sides(names),
                        notes,
                        *kept,
                        *arrived,
                        scalars=1,
                    )
                notes = outs[-1]
                for k in range(2):
                    left[k].remove(names[k])
                if joined:
                    move = lambda a: lax.ppermute(a, bits[0], SWAP)
                    return outs[1], travel(outs[0], kind, move), notes
                kept = outs[2:4]
                casts = [a.astype(jnp.float16) if kind is Scale else a for a in outs[0:2]]
                moved = [lax.ppermute(a, name, SWAP) for a, name in zip(casts, names)]
                arrived = [a.astype(F32) if kind is Scale else a for a in moved]

        full = ((height, cases), F32)
        start, sent = call(first_body, [full, ((height + EXTRA, cases), F32)], right, precond)
        kept, got, _ = exchange(gather(sent, Scale), Scale)
        work, sent = call(
            second_body, [full, ((height + EXTRA, cases), BF16)], kept, got, start, precond
        )
        kept, got, notes = exchange(gather(sent, Sums), Sums)
        side, flat, notes = call(
            third_body,
            [full, ((4 * cases // 128, 128), F32), ((NOTE, cases), F32)],
            kept,
            got,
            notes,
            start,
            work,
            precond,
        )
        flat = flat + lax.ppermute(flat, "core", SWAP)
        members = sources // 2 * 2 ** len(bits)
        flat = lax.all_to_all(
            jnp.broadcast_to(flat, (members,) + flat.shape), ("row",) + tuple(bits), 0, 0
        )
        answer, arnoldi = call(last_body, [full, ((6, cases), F32)], flat, notes, start, side)
        return answer.reshape(3, node_dev, cases), arnoldi.reshape(3, 2, cases)

    return local


def solution(mesh):
    count_tgt, count_src = mesh.shape["tgt"], mesh.shape["src"]
    depth = count_src.bit_length() - 1
    bits = ["bit%d" % k for k in reversed(range(depth))]
    tgt = ("row", "core")
    src = tuple(bits)
    grid = mesh.devices.reshape((count_tgt // 2, 2) + (2,) * depth)
    placed = (
        P(None, None, None, src, None, tgt),
        P(None, tgt + src, None),
        P(None, tgt + src),
    )
    return jax.shard_map(
        build(bits),
        mesh=Mesh(grid, tgt + src),
        in_specs=placed,
        out_specs=(P(None, tgt + src, None), P()),
        check_vma=False,
    )
```

```python
import functools

import jax
import jax.numpy as jnp
from jax import lax
from jax.experimental import pallas as pl
from jax.experimental.pallas import tpu as pltpu
from jax.sharding import Mesh, PartitionSpec as P

FIBER_NODES = 32
PIECES = 3
EXTRA = 16
NOTE = 8
SWAP = [(0, 1), (1, 0)]
TINY = 1e-06
F32 = jnp.float32
BF16 = jnp.bfloat16


def least_squares(beta, h_one_one, h_two_one, h_one_two, h_two_two, h_three_two):
    rho_one = jnp.sqrt(h_one_one * h_one_one + h_two_one * h_two_one)
    cos_one = h_one_one / rho_one
    sin_one = h_two_one / rho_one
    g_one = cos_one * beta
    g_two = -sin_one * beta
    top = cos_one * h_one_two + sin_one * h_two_two
    low = cos_one * h_two_two - sin_one * h_one_two
    rho_two = jnp.sqrt(low * low + h_three_two * h_three_two)
    cos_two = low / rho_two
    sin_two = h_three_two / rho_two
    y_two = cos_two * g_two / rho_two
    y_one = (g_one - top * y_two) / rho_one
    return (y_one, y_two, jnp.abs(sin_two * g_two))


def stack_rows(rows, count):
    blank = jnp.zeros_like(rows[0])
    return jnp.concatenate(list(rows) + [blank] * (count - len(rows)), axis=0)


class Scale:
    sent = F32

    def __init__(self, size):
        factors = []
        scale = jnp.ones_like(size)
        rest = size
        for _ in range(PIECES):
            factor = jnp.clip(rest, 2.0**-13, 2.0**15).astype(BF16).astype(F32)
            factors.append(factor)
            scale = scale * factor
            rest = rest / factor
        self.scale = scale
        self.inverse = 1.0 / scale
        self.packed = stack_rows(factors, EXTRA)

    def pack(self, body):
        return body * self.inverse

    @staticmethod
    def read(rows):
        return rows[0:1] * rows[1:2] * rows[2:3]

    @staticmethod
    def unpack(body, other):
        return body * other

    @classmethod
    def load(cls, note):
        return cls(note[0:1, :])

    def merge(self, other):
        return Scale(jnp.maximum(self.scale, other))

    def rows(self):
        return stack_rows([self.scale], NOTE)


class Sums:
    sent = BF16

    def __init__(self, total):
        pieces = []
        rest = total
        for _ in range(PIECES):
            piece = rest.astype(BF16).astype(F32)
            pieces.append(piece)
            rest = rest - piece
        self.total = total
        rows = [piece[k : k + 1] for piece in pieces for k in range(2)]
        self.packed = stack_rows(rows, EXTRA).astype(BF16)

    def pack(self, body):
        return body.astype(BF16)

    @staticmethod
    def read(rows):
        wide = rows.astype(F32)
        return wide[0:2] + wide[2:4] + wide[4:6]

    @staticmethod
    def unpack(body, other):
        return body.astype(F32)

    @classmethod
    def load(cls, note):
        return cls(note[0:2, :])

    def merge(self, other):
        return Sums(self.total + other)

    def rows(self):
        return stack_rows([self.total[0:1], self.total[1:2]], NOTE)


def insert(slot, place, side):
    low = slot & ((1 << place) - 1)
    return ((slot >> place) << (place + 1)) + (side << place) + low


def blocks_times(precond, value):
    width = 3 * FIBER_NODES
    fibers = precond.shape[1] // width
    nodes = fibers * FIBER_NODES
    results = []
    for fiber in range(fibers):
        parts = []
        for comp in range(3):
            first = comp * nodes + fiber * FIBER_NODES
            parts.append(value[first : first + FIBER_NODES])
        column = jnp.concatenate(parts, axis=0)
        blank = jnp.zeros_like(column)
        tall = [column if k == fiber else blank for k in range(fibers)]
        results.append(
            jnp.dot(
                precond,
                jnp.concatenate(tall, axis=0),
                precision=lax.Precision.HIGHEST,
                preferred_element_type=F32,
            )
        )
    parts = []
    for comp in range(3):
        for fiber in range(fibers):
            parts.append(results[fiber][comp * FIBER_NODES : (comp + 1) * FIBER_NODES])
    return jnp.concatenate(parts, axis=0)


def row_sum(first, second):
    return jnp.sum(first * second, axis=0, keepdims=True)


def first_body(right_ref, precond_ref, start_ref, sent_ref):
    height = start_ref.shape[0]
    start = blocks_times(precond_ref[...], right_ref[...])
    start_ref[...] = start
    note = Scale(jnp.max(jnp.abs(start), axis=0, keepdims=True))
    sent_ref[0:height] = note.pack(start)
    sent_ref[height:] = note.packed


def couple_body(kind, places, sides_ref, tile_ref, got_ref, *refs):
    sends, keeps, note_ref, work_ref = refs[0:2], refs[2:4], refs[4], refs[5]
    sources = got_ref.shape[0]
    height = got_ref.shape[1] - EXTRA
    nodes = height // 3
    cases = got_ref.shape[2]
    half = cases // 2
    targets = tile_ref.shape[3] // nodes
    others = [kind.read(got_ref[k, height:]) for k in range(sources)]
    blocks = []
    for comp in range(3):
        for k in range(sources):
            block = got_ref[k, comp * nodes : (comp + 1) * nodes]
            if kind is Scale:
                block = block * others[k]
            blocks.append(block)
    value = jnp.concatenate(blocks, axis=0)
    terms = [value.astype(BF16)]
    if kind is Scale:
        note = Scale(functools.reduce(jnp.maximum, others))
        terms.append((value - terms[0].astype(F32)).astype(BF16))
    else:
        note = Sums(functools.reduce(jnp.add, others))
    note_ref[...] = note.rows()
    for comp in range(3):
        left = tile_ref[:, comp].reshape(value.shape[0], targets * nodes)
        total = 0.0
        for term in terms:
            total = total + lax.dot_general(
                left, term, (((0,), (0,)), ((), ())), preferred_element_type=F32
            )
        work_ref[comp] = total
    for colour in range(2):
        first = colour * half
        columns = slice(first, first + half)
        side = sides_ref[colour]
        inner_note = type(note).load(note_ref[:, columns])
        for slot in range(targets // 2):
            give = insert(slot, places[colour], 1 - side) * nodes
            keep = insert(slot, places[colour], side) * nodes
            for comp in range(3):
                row = slot * height + comp * nodes
                value = work_ref[comp, pl.ds(pl.multiple_of(give, nodes), nodes), columns]
                sends[colour][row : row + nodes] = inner_note.pack(value)
                value = work_ref[comp, pl.ds(pl.multiple_of(keep, nodes), nodes), columns]
                keeps[colour][row : row + nodes] = value
        sends[colour][targets // 2 * height :] = inner_note.packed


def merge_body(kind, places, joined, height, sides_ref, note_ref, *refs):
    kept, got, outs, next_ref = refs[0:2], refs[2:4], refs[4:-1], refs[-1]
    half = kept[0].shape[1]
    slots = kept[0].shape[0] // height
    for colour in range(2):
        columns = slice(colour * half, (colour + 1) * half)
        side = sides_ref[colour]
        other = kind.read(got[colour][slots * height :])
        note = kind.load(note_ref[:, columns]).merge(other)
        next_ref[:, columns] = note.rows()
        for slot in range(slots // 2):
            rows = slice(slot * height, (slot + 1) * height)
            give = pl.ds(pl.multiple_of(insert(slot, places[colour], 1 - side) * height, height), height)
            keep = pl.ds(pl.multiple_of(insert(slot, places[colour], side) * height, height), height)
            given = note.pack(kept[colour][give] + kind.unpack(got[colour][give], other))
            held = kept[colour][keep] + kind.unpack(got[colour][keep], other)
            if joined:
                outs[0][rows, columns] = given
                outs[1][rows, columns] = held
            else:
                outs[colour][rows] = given
                outs[2 + colour][rows] = held
        if joined:
            outs[0][slots // 2 * height :, columns] = note.packed
        else:
            outs[colour][slots // 2 * height :] = note.packed


def second_body(kept_ref, got_ref, start_ref, precond_ref, work_ref, sent_ref):
    height = start_ref.shape[0]
    other = Scale.read(got_ref[height:])
    start = start_ref[...]
    moved = start + (kept_ref[...] + Scale.unpack(got_ref[0:height], other))
    work = blocks_times(precond_ref[...], moved)
    work_ref[...] = work
    note = Sums(jnp.concatenate([row_sum(start, start), row_sum(start, work)], axis=0))
    sent_ref[0:height] = note.pack(work)
    sent_ref[height:] = note.packed


def third_body(kept_ref, got_ref, note_ref, start_ref, work_ref, precond_ref, side_ref, gram_ref, next_ref):
    height = start_ref.shape[0]
    note = Sums.load(note_ref[...]).merge(Sums.read(got_ref[height:]))
    next_ref[...] = note.rows()
    start = start_ref[...]
    work = work_ref[...]
    moved = work + (kept_ref[...] + got_ref[0:height].astype(F32))
    h_one_one = note.total[1:2] / (note.total[0:1] + TINY)
    other = blocks_times(precond_ref[...], moved) - h_one_one * work
    side = work - h_one_one * start
    side_ref[...] = side
    pairs = [(side, side), (start, other), (side, other), (other, other)]
    rows = [row_sum(*pair) for pair in pairs]
    width = gram_ref.shape[1]
    count = rows[0].shape[1] // width
    parts = [row[:, k * width : (k + 1) * width] for row in rows for k in range(count)]
    gram_ref[...] = jnp.concatenate(parts, axis=0)


def last_body(flat_ref, note_ref, start_ref, side_ref, solution_ref, arnoldi_ref):
    total = jnp.sum(flat_ref[...], axis=0)
    count = total.shape[0] // 4
    gram = [
        jnp.concatenate([total[k * count + q : k * count + q + 1] for q in range(count)], axis=1)
        for k in range(4)
    ]
    side_side, start_other, side_other, other_other = gram
    square = note_ref[0:1, :] + TINY
    beta = jnp.sqrt(square)
    h_one_one = note_ref[1:2, :] / square
    h_two_one = jnp.sqrt(side_side / square + TINY)
    length = beta * h_two_one
    h_one_two = start_other / (beta * length)
    h_two_two = side_other / (length * length)
    loss_one = TINY / square
    loss_two = TINY / (h_two_one * h_two_one)
    one_two = h_one_one * loss_one / h_two_one
    rest = (
        other_other / (length * length)
        - h_one_two * h_one_two * (1.0 + loss_one)
        - h_two_two * h_two_two * (1.0 + loss_two)
        + 2.0 * h_one_two * h_two_two * one_two
    )
    h_three_two = jnp.sqrt(jnp.maximum(rest, 0.0) + TINY)
    y_one, y_two, estimate = least_squares(
        beta, h_one_one, h_two_one, h_one_two, h_two_two, h_three_two
    )
    solution_ref[...] = (y_one / beta) * start_ref[...] + (y_two / length) * side_ref[...]
    rows = [h_one_one, h_one_two, h_two_one, h_two_two, estimate, h_three_two]
    arnoldi_ref[...] = jnp.concatenate(rows, axis=0)


def call(body, shapes, *args, scalars=0, outside=0, scratch=()):
    spec = pl.BlockSpec(memory_space=pltpu.VMEM)
    small = pl.BlockSpec(memory_space=pltpu.SMEM)
    held = [pltpu.with_memory_space_constraint(arg, pltpu.VMEM) for arg in args[scalars:]]
    inside = len(shapes) - outside
    return pl.pallas_call(
        body,
        out_shape=[pltpu.VMEM(shape, dtype) for shape, dtype in shapes[:inside]]
        + [jax.ShapeDtypeStruct(shape, dtype) for shape, dtype in shapes[inside:]],
        in_specs=[small] * scalars + [spec] * len(held),
        out_specs=[spec] * len(shapes),
        scratch_shapes=list(scratch),
        compiler_params=pltpu.CompilerParams(vmem_limit_bytes=24 * 1024 * 1024),
    )(*args[:scalars], *held)


def travel(array, kind, move):
    if kind is Scale:
        return move(array.astype(jnp.float16)).astype(F32)
    return move(array)


def build(bits):
    lower = bits[1:]
    orders = (list(reversed(lower)), list(lower))

    def local(mobility, right_side, precond):
        row_count = mobility.shape[5]
        sources = mobility.shape[2]
        node_dev = mobility.shape[4]
        cases = right_side.shape[2]
        height = 3 * node_dev
        half = cases // 2
        tile = mobility.reshape(3, 3, sources * node_dev, row_count)
        right = right_side.reshape(height, cases)

        def sides(names):
            return jnp.stack([lax.axis_index(name).astype(jnp.int32) for name in names])

        def gather(sent, kind):
            return travel(sent, kind, lambda a: lax.all_gather(a, ("row", "core")))

        def exchange(got, kind):
            left = [list(bits), list(bits)]
            slots = row_count // node_dev
            for step in range(len(lower) + 1):
                joined = step == len(lower)
                names = [bits[0]] * 2 if joined else [orders[0][step], orders[1][step]]
                places = [len(left[k]) - 1 - left[k].index(names[k]) for k in range(2)]
                slots = slots // 2
                tall = slots * height
                note = ((NOTE, cases), F32)
                if step == 0:
                    shapes = [((tall + EXTRA, half), kind.sent)] * 2 + [((tall, half), F32)] * 2
                    outs = call(
                        functools.partial(couple_body, kind, places),
                        shapes + [note],
                        sides(names),
                        tile,
                        got,
                        scalars=1,
                        scratch=[pltpu.VMEM((3, row_count, cases), F32)],
                    )
                else:
                    shapes = [((tall + EXTRA, half), kind.sent)] * 2 + [((tall, half), F32)] * 2
                    if joined:
                        shapes = [((tall + EXTRA, cases), kind.sent), ((tall, cases), F32)]
                    outs = call(
                        functools.partial(merge_body, kind, places, joined, height),
                        shapes + [note],
                        sides(names),
                        notes,
                        *kept,
                        *arrived,
                        scalars=1,
                    )
                notes = outs[-1]
                for k in range(2):
                    left[k].remove(names[k])
                if joined:
                    move = lambda a: lax.ppermute(a, bits[0], SWAP)
                    return outs[1], travel(outs[0], kind, move), notes
                kept = outs[2:4]
                casts = [a.astype(jnp.float16) if kind is Scale else a for a in outs[0:2]]
                moved = [lax.ppermute(a, name, SWAP) for a, name in zip(casts, names)]
                arrived = [a.astype(F32) if kind is Scale else a for a in moved]

        full = ((height, cases), F32)
        start, sent = call(first_body, [full, ((height + EXTRA, cases), F32)], right, precond)
        kept, got, _ = exchange(gather(sent, Scale), Scale)
        work, sent = call(
            second_body, [full, ((height + EXTRA, cases), BF16)], kept, got, start, precond
        )
        kept, got, notes = exchange(gather(sent, Sums), Sums)
        side, flat, notes = call(
            third_body,
            [full, ((4 * cases // 128, 128), F32), ((NOTE, cases), F32)],
            kept,
            got,
            notes,
            start,
            work,
            precond,
        )
        flat = flat + lax.ppermute(flat, "core", SWAP)
        members = sources // 2 * 2 ** len(bits)
        flat = lax.all_to_all(
            jnp.broadcast_to(flat, (members,) + flat.shape), ("row",) + tuple(bits), 0, 0
        )
        answer, arnoldi = call(last_body, [full, ((6, cases), F32)], flat, notes, start, side, outside=2)
        return answer.reshape(3, node_dev, cases), arnoldi.reshape(3, 2, cases)

    return local


def solution(mesh):
    count_tgt, count_src = mesh.shape["tgt"], mesh.shape["src"]
    depth = count_src.bit_length() - 1
    bits = ["bit%d" % k for k in reversed(range(depth))]
    tgt = ("row", "core")
    src = tuple(bits)
    grid = mesh.devices.reshape((count_tgt // 2, 2) + (2,) * depth)
    placed = (
        P(None, None, None, src, None, tgt),
        P(None, tgt + src, None),
        P(None, tgt + src),
    )
    return jax.shard_map(
        build(bits),
        mesh=Mesh(grid, tgt + src),
        in_specs=placed,
        out_specs=(P(None, tgt + src, None), P()),
        check_vma=False,
    )
```

```python
import functools

import jax
import jax.numpy as jnp
from jax import lax
from jax.experimental import pallas as pl
from jax.experimental.pallas import tpu as pltpu
from jax.sharding import Mesh, PartitionSpec as P

FIBER_NODES = 32
PIECES = 3
EXTRA = 16
NOTE = 8
SWAP = [(0, 1), (1, 0)]
TINY = 1e-06
F32 = jnp.float32
BF16 = jnp.bfloat16


def least_squares(beta, h_one_one, h_two_one, h_one_two, h_two_two, h_three_two):
    rho_one = jnp.sqrt(h_one_one * h_one_one + h_two_one * h_two_one)
    cos_one = h_one_one / rho_one
    sin_one = h_two_one / rho_one
    g_one = cos_one * beta
    g_two = -sin_one * beta
    top = cos_one * h_one_two + sin_one * h_two_two
    low = cos_one * h_two_two - sin_one * h_one_two
    rho_two = jnp.sqrt(low * low + h_three_two * h_three_two)
    cos_two = low / rho_two
    sin_two = h_three_two / rho_two
    y_two = cos_two * g_two / rho_two
    y_one = (g_one - top * y_two) / rho_one
    return (y_one, y_two, jnp.abs(sin_two * g_two))


def stack_rows(rows, count):
    blank = jnp.zeros_like(rows[0])
    return jnp.concatenate(list(rows) + [blank] * (count - len(rows)), axis=0)


class Scale:
    sent = F32

    def __init__(self, size):
        factors = []
        scale = jnp.ones_like(size)
        rest = size
        for _ in range(PIECES):
            factor = jnp.clip(rest, 2.0**-13, 2.0**15).astype(BF16).astype(F32)
            factors.append(factor)
            scale = scale * factor
            rest = rest / factor
        self.scale = scale
        self.inverse = 1.0 / scale
        self.packed = stack_rows(factors, EXTRA)

    def pack(self, body):
        return body * self.inverse

    @staticmethod
    def read(rows):
        return rows[0:1] * rows[1:2] * rows[2:3]

    @staticmethod
    def unpack(body, other):
        return body * other

    @classmethod
    def load(cls, note):
        return cls(note[0:1, :])

    def merge(self, other):
        return Scale(jnp.maximum(self.scale, other))

    def rows(self):
        return stack_rows([self.scale], NOTE)


class Sums:
    sent = BF16

    def __init__(self, total):
        pieces = []
        rest = total
        for _ in range(PIECES):
            piece = rest.astype(BF16).astype(F32)
            pieces.append(piece)
            rest = rest - piece
        self.total = total
        rows = [piece[k : k + 1] for piece in pieces for k in range(2)]
        self.packed = stack_rows(rows, EXTRA).astype(BF16)

    def pack(self, body):
        return body.astype(BF16)

    @staticmethod
    def read(rows):
        wide = rows.astype(F32)
        return wide[0:2] + wide[2:4] + wide[4:6]

    @staticmethod
    def unpack(body, other):
        return body.astype(F32)

    @classmethod
    def load(cls, note):
        return cls(note[0:2, :])

    def merge(self, other):
        return Sums(self.total + other)

    def rows(self):
        return stack_rows([self.total[0:1], self.total[1:2]], NOTE)


def insert(slot, place, side):
    low = slot & ((1 << place) - 1)
    return ((slot >> place) << (place + 1)) + (side << place) + low


def blocks_times(precond, value):
    width = 3 * FIBER_NODES
    fibers = precond.shape[1] // width
    nodes = fibers * FIBER_NODES
    results = []
    for fiber in range(fibers):
        parts = []
        for comp in range(3):
            first = comp * nodes + fiber * FIBER_NODES
            parts.append(value[first : first + FIBER_NODES])
        column = jnp.concatenate(parts, axis=0)
        blank = jnp.zeros_like(column)
        tall = [column if k == fiber else blank for k in range(fibers)]
        results.append(
            jnp.dot(
                precond,
                jnp.concatenate(tall, axis=0),
                precision=lax.Precision.HIGHEST,
                preferred_element_type=F32,
            )
        )
    parts = []
    for comp in range(3):
        for fiber in range(fibers):
            parts.append(results[fiber][comp * FIBER_NODES : (comp + 1) * FIBER_NODES])
    return jnp.concatenate(parts, axis=0)


def row_sum(first, second):
    return jnp.sum(first * second, axis=0, keepdims=True)


def first_body(right_ref, precond_ref, start_ref, sent_ref):
    height = start_ref.shape[0]
    start = blocks_times(precond_ref[...], right_ref[...])
    start_ref[...] = start
    note = Scale(jnp.max(jnp.abs(start), axis=0, keepdims=True))
    sent_ref[0:height] = note.pack(start)
    sent_ref[height:] = note.packed


def couple_body(kind, places, sides_ref, tile_ref, got_ref, *refs):
    sends, keeps, note_ref, work_ref = refs[0:4], refs[4:8], refs[8], refs[9]
    sources = got_ref.shape[0]
    height = got_ref.shape[1] - EXTRA
    nodes = height // 3
    cases = got_ref.shape[2]
    half = cases // 2
    targets = tile_ref.shape[3] // nodes
    others = [kind.read(got_ref[k, height:]) for k in range(sources)]
    blocks = []
    for comp in range(3):
        for k in range(sources):
            block = got_ref[k, comp * nodes : (comp + 1) * nodes]
            if kind is Scale:
                block = block * others[k]
            blocks.append(block)
    value = jnp.concatenate(blocks, axis=0)
    terms = [value.astype(BF16)]
    if kind is Scale:
        note = Scale(functools.reduce(jnp.maximum, others))
        terms.append((value - terms[0].astype(F32)).astype(BF16))
    else:
        note = Sums(functools.reduce(jnp.add, others))
    note_ref[...] = note.rows()
    for comp in range(3):
        left = tile_ref[:, comp].reshape(value.shape[0], targets * nodes)
        total = 0.0
        for term in terms:
            total = total + lax.dot_general(
                left, term, (((0,), (0,)), ((), ())), preferred_element_type=F32
            )
        work_ref[comp] = total
    slots = targets // 4
    top = sides_ref[2]
    for colour in range(2):
        first = colour * half
        columns = slice(first, first + half)
        side = sides_ref[colour]
        inner_note = type(note).load(note_ref[:, columns])
        for near in range(2):
            base = (top if near else 1 - top) * (targets // 2)
            send, kept = sends[near * 2 + colour], keeps[near * 2 + colour]
            for slot in range(slots):
                give = (base + insert(slot, places[colour], 1 - side)) * nodes
                keep = (base + insert(slot, places[colour], side)) * nodes
                for comp in range(3):
                    row = slot * height + comp * nodes
                    value = work_ref[comp, pl.ds(pl.multiple_of(give, nodes), nodes), columns]
                    send[row : row + nodes] = inner_note.pack(value)
                    value = work_ref[comp, pl.ds(pl.multiple_of(keep, nodes), nodes), columns]
                    kept[row : row + nodes] = value
            send[slots * height :] = inner_note.packed


def merge_body(kind, places, height, sides_ref, note_ref, *refs):
    kept, got, outs, next_ref = refs[0:2], refs[2:4], refs[4:8], refs[8]
    half = kept[0].shape[1]
    slots = kept[0].shape[0] // height
    for colour in range(2):
        columns = slice(colour * half, (colour + 1) * half)
        side = sides_ref[colour]
        other = kind.read(got[colour][slots * height :])
        note = kind.load(note_ref[:, columns]).merge(other)
        next_ref[:, columns] = note.rows()
        for slot in range(slots // 2):
            rows = slice(slot * height, (slot + 1) * height)
            give = pl.ds(pl.multiple_of(insert(slot, places[colour], 1 - side) * height, height), height)
            keep = pl.ds(pl.multiple_of(insert(slot, places[colour], side) * height, height), height)
            outs[colour][rows] = note.pack(kept[colour][give] + kind.unpack(got[colour][give], other))
            outs[2 + colour][rows] = kept[colour][keep] + kind.unpack(got[colour][keep], other)
        outs[colour][slots // 2 * height :] = note.packed


def join_body(kind, note_ref, *refs):
    kept, got, sent_ref, next_ref = refs[0:2], refs[2:4], refs[4], refs[5]
    height, half = kept[0].shape
    for colour in range(2):
        columns = slice(colour * half, (colour + 1) * half)
        other = kind.read(got[colour][height:])
        note = kind.load(note_ref[:, columns]).merge(other)
        next_ref[:, columns] = note.rows()
        sent_ref[0:height, columns] = note.pack(
            kept[colour][...] + kind.unpack(got[colour][0:height], other)
        )
        sent_ref[height:, columns] = note.packed


def share_of(kind, kept, got, far_ref):
    height = kept[0].shape[0]
    parts = []
    for colour in range(2):
        other = kind.read(got[colour][height:])
        parts.append(kept[colour][...] + kind.unpack(got[colour][0:height], other))
    other = kind.read(far_ref[height:])
    return jnp.concatenate(parts, axis=1) + kind.unpack(far_ref[0:height], other), other


def second_body(*refs):
    kept, got, far_ref = refs[0:2], refs[2:4], refs[4]
    start_ref, precond_ref, work_ref, sent_ref = refs[5:]
    height = start_ref.shape[0]
    start = start_ref[...]
    share, _ = share_of(Scale, kept, got, far_ref)
    work = blocks_times(precond_ref[...], start + share)
    work_ref[...] = work
    note = Sums(jnp.concatenate([row_sum(start, start), row_sum(start, work)], axis=0))
    sent_ref[0:height] = note.pack(work)
    sent_ref[height:] = note.packed


def third_body(*refs):
    kept, got, far_ref = refs[0:2], refs[2:4], refs[4]
    note_ref, start_ref, work_ref, precond_ref, side_ref, gram_ref, next_ref = refs[5:]
    share, sums = share_of(Sums, kept, got, far_ref)
    note = Sums.load(note_ref[...]).merge(sums)
    next_ref[...] = note.rows()
    start = start_ref[...]
    work = work_ref[...]
    h_one_one = note.total[1:2] / (note.total[0:1] + TINY)
    other = blocks_times(precond_ref[...], work + share) - h_one_one * work
    side = work - h_one_one * start
    side_ref[...] = side
    pairs = [(side, side), (start, other), (side, other), (other, other)]
    rows = [row_sum(*pair) for pair in pairs]
    width = gram_ref.shape[1]
    count = rows[0].shape[1] // width
    parts = [row[:, k * width : (k + 1) * width] for row in rows for k in range(count)]
    gram_ref[...] = jnp.concatenate(parts, axis=0)


def last_body(flat_ref, note_ref, start_ref, side_ref, solution_ref, arnoldi_ref):
    total = jnp.sum(flat_ref[...], axis=0)
    count = total.shape[0] // 4
    gram = [
        jnp.concatenate([total[k * count + q : k * count + q + 1] for q in range(count)], axis=1)
        for k in range(4)
    ]
    side_side, start_other, side_other, other_other = gram
    square = note_ref[0:1, :] + TINY
    beta = jnp.sqrt(square)
    h_one_one = note_ref[1:2, :] / square
    h_two_one = jnp.sqrt(side_side / square + TINY)
    length = beta * h_two_one
    h_one_two = start_other / (beta * length)
    h_two_two = side_other / (length * length)
    loss_one = TINY / square
    loss_two = TINY / (h_two_one * h_two_one)
    one_two = h_one_one * loss_one / h_two_one
    rest = (
        other_other / (length * length)
        - h_one_two * h_one_two * (1.0 + loss_one)
        - h_two_two * h_two_two * (1.0 + loss_two)
        + 2.0 * h_one_two * h_two_two * one_two
    )
    h_three_two = jnp.sqrt(jnp.maximum(rest, 0.0) + TINY)
    y_one, y_two, estimate = least_squares(
        beta, h_one_one, h_two_one, h_one_two, h_two_two, h_three_two
    )
    solution_ref[...] = (y_one / beta) * start_ref[...] + (y_two / length) * side_ref[...]
    arnoldi_ref[0] = jnp.concatenate([h_one_one, h_one_two], axis=0)
    arnoldi_ref[1] = jnp.concatenate([h_two_one, h_two_two], axis=0)
    arnoldi_ref[2] = jnp.concatenate([estimate, h_three_two], axis=0)


def call(body, shapes, *args, scalars=0, outside=0, scratch=(), hold=True):
    spec = pl.BlockSpec(memory_space=pltpu.VMEM)
    small = pl.BlockSpec(memory_space=pltpu.SMEM)
    held = list(args[scalars:])
    if hold:
        held = [pltpu.with_memory_space_constraint(arg, pltpu.VMEM) for arg in held]
    inside = len(shapes) - outside
    return pl.pallas_call(
        body,
        out_shape=[pltpu.VMEM(shape, dtype) for shape, dtype in shapes[:inside]]
        + [jax.ShapeDtypeStruct(shape, dtype) for shape, dtype in shapes[inside:]],
        in_specs=[small] * scalars + [spec] * len(held),
        out_specs=[spec] * len(shapes),
        scratch_shapes=list(scratch),
        compiler_params=pltpu.CompilerParams(vmem_limit_bytes=20 * 1024 * 1024),
    )(*args[:scalars], *held)


def travel(array, kind, move):
    if kind is Scale:
        return move(array.astype(jnp.float16)).astype(F32)
    return move(array)


def build(bits):
    lower = bits[1:]
    orders = (list(reversed(lower)), list(lower))

    def local(mobility, right_side, precond):
        row_count = mobility.shape[5]
        sources = mobility.shape[2]
        node_dev = mobility.shape[4]
        cases = right_side.shape[2]
        height = 3 * node_dev
        half = cases // 2
        tile = mobility.reshape(3, 3, sources * node_dev, row_count)
        right = right_side.reshape(height, cases)

        def sides(names):
            return jnp.stack([lax.axis_index(name).astype(jnp.int32) for name in names])

        def gather(sent, kind):
            return travel(sent, kind, lambda a: lax.all_gather(a, ("row", "core")))

        def cast(array, kind):
            return array.astype(jnp.float16) if kind is Scale else array

        def widen(array, kind):
            return array.astype(F32) if kind is Scale else array

        def swap(arrays, names, kind):
            moved = [lax.ppermute(cast(a, kind), name, SWAP) for a, name in zip(arrays, names)]
            return [widen(a, kind) for a in moved]

        def exchange(got, kind):
            left = [list(lower), list(lower)]
            note = ((NOTE, cases), F32)
            slots = row_count // node_dev // 2

            def take(step):
                names = [orders[0][step], orders[1][step]]
                places = [len(left[k]) - 1 - left[k].index(names[k]) for k in range(2)]
                for k in range(2):
                    left[k].remove(names[k])
                return names, places

            def shapes(count):
                tall = count * height
                return [((tall + EXTRA, half), kind.sent)], [((tall, half), F32)]

            names, places = take(0)
            slots = slots // 2
            sent, kept = shapes(slots)
            outs = call(
                functools.partial(couple_body, kind, places),
                sent * 4 + kept * 4 + [note],
                sides(names + [bits[0]]),
                tile,
                got,
                scalars=1,
                scratch=[pltpu.VMEM((3, row_count, cases), F32)],
            )
            near = [outs[2:4], outs[6:8], outs[8]]
            far = [outs[0:2], outs[4:6], outs[8]]
            plan = [(names, None)]
            for step in range(1, len(lower)):
                plan.append(take(step))

            def reduce(state, tie):
                count = slots
                sends, kept, notes = state
                arrived = swap(sends, plan[0][0], kind)
                for names, places in plan[1:]:
                    count = count // 2
                    sent, keep = shapes(count)
                    outs = call(
                        functools.partial(merge_body, kind, places, height),
                        sent * 2 + keep * 2 + [note],
                        sides(names),
                        notes,
                        *kept,
                        *arrived,
                        scalars=1,
                    )
                    if tie is not None:
                        tie.append(outs[4])
                    kept, notes = outs[2:4], outs[4]
                    arrived = swap(outs[0:2], names, kind)
                return kept, arrived, notes

            ties = []
            kept, arrived, notes = reduce(far, ties)
            sent, notes = call(
                functools.partial(join_body, kind),
                [((height + EXTRA, cases), kind.sent), note],
                notes,
                *kept,
                *arrived,
            )
            if ties:
                tied = lax.optimization_barrier(tuple(near[0]) + (ties[0],))
                near[0] = list(tied[:2])
            (crossed,) = swap([sent], [bits[0]], kind)
            kept, arrived, _ = reduce(near, None)
            return list(kept) + list(arrived) + [crossed], notes

        full = ((height, cases), F32)
        packed = ((height + EXTRA, cases), F32)
        start, sent = call(first_body, [full, packed], right, precond, hold=False)
        shares, _ = exchange(gather(sent, Scale), Scale)
        packed = ((height + EXTRA, cases), BF16)
        work, sent = call(second_body, [full, packed], *shares, start, precond)
        shares, notes = exchange(gather(sent, Sums), Sums)
        side, flat, notes = call(
            third_body,
            [full, ((4 * cases // 128, 128), F32), ((NOTE, cases), F32)],
            *shares,
            notes,
            start,
            work,
            precond,
        )
        flat = flat + lax.ppermute(flat, "core", SWAP)
        members = sources // 2 * 2 ** len(bits)
        flat = lax.all_to_all(
            jnp.broadcast_to(flat, (members,) + flat.shape), ("row",) + tuple(bits), 0, 0
        )
        answer, arnoldi = call(last_body, [full, ((3, 2, cases), F32)], flat, notes, start, side, outside=2)
        return answer.reshape(3, node_dev, cases), arnoldi

    return local


def solution(mesh):
    count_tgt, count_src = mesh.shape["tgt"], mesh.shape["src"]
    depth = count_src.bit_length() - 1
    bits = ["bit%d" % k for k in reversed(range(depth))]
    tgt = ("row", "core")
    src = tuple(bits)
    grid = mesh.devices.reshape((count_tgt // 2, 2) + (2,) * depth)
    placed = (
        P(None, None, None, src, None, tgt),
        P(None, tgt + src, None),
        P(None, tgt + src),
    )
    return jax.shard_map(
        build(bits),
        mesh=Mesh(grid, tgt + src),
        in_specs=placed,
        out_specs=(P(None, tgt + src, None), P()),
        check_vma=False,
    )
```

```python
import functools

import jax
import jax.numpy as jnp
from jax import lax
from jax.experimental import pallas as pl
from jax.experimental.pallas import tpu as pltpu
from jax.sharding import Mesh, PartitionSpec as P

FIBER_NODES = 32
PIECES = 3
EXTRA = 8
NOTE = 8
SWAP = [(0, 1), (1, 0)]
TINY = 1e-06
F32 = jnp.float32
BF16 = jnp.bfloat16


def least_squares(beta, h_one_one, h_two_one, h_one_two, h_two_two, h_three_two):
    rho_one = jnp.sqrt(h_one_one * h_one_one + h_two_one * h_two_one)
    cos_one = h_one_one / rho_one
    sin_one = h_two_one / rho_one
    g_one = cos_one * beta
    g_two = -sin_one * beta
    top = cos_one * h_one_two + sin_one * h_two_two
    low = cos_one * h_two_two - sin_one * h_one_two
    rho_two = jnp.sqrt(low * low + h_three_two * h_three_two)
    cos_two = low / rho_two
    sin_two = h_three_two / rho_two
    y_two = cos_two * g_two / rho_two
    y_one = (g_one - top * y_two) / rho_one
    return (y_one, y_two, jnp.abs(sin_two * g_two))


def stack_rows(rows, count):
    blank = jnp.zeros_like(rows[0])
    return jnp.concatenate(list(rows) + [blank] * (count - len(rows)), axis=0)


class Scale:
    sent = F32

    def __init__(self, size):
        factors = []
        scale = jnp.ones_like(size)
        rest = size
        for _ in range(PIECES):
            factor = jnp.clip(rest, 2.0**-13, 2.0**15).astype(BF16).astype(F32)
            factors.append(factor)
            scale = scale * factor
            rest = rest / factor
        self.scale = scale
        self.inverse = 1.0 / scale
        self.packed = stack_rows(factors, EXTRA)

    def pack(self, body):
        return body * self.inverse

    @staticmethod
    def read(rows):
        return rows[0:1] * rows[1:2] * rows[2:3]

    @staticmethod
    def unpack(body, other):
        return body * other

    @classmethod
    def load(cls, note):
        return cls(note[0:1, :])

    def merge(self, other):
        return Scale(jnp.maximum(self.scale, other))

    def rows(self):
        return stack_rows([self.scale], NOTE)


class Sums:
    sent = BF16

    def __init__(self, total):
        pieces = []
        rest = total
        for _ in range(PIECES):
            piece = rest.astype(BF16).astype(F32)
            pieces.append(piece)
            rest = rest - piece
        self.total = total
        rows = [piece[k : k + 1] for piece in pieces for k in range(2)]
        self.packed = stack_rows(rows, EXTRA).astype(BF16)

    def pack(self, body):
        return body.astype(BF16)

    @staticmethod
    def read(rows):
        wide = rows.astype(F32)
        return wide[0:2] + wide[2:4] + wide[4:6]

    @staticmethod
    def unpack(body, other):
        return body.astype(F32)

    @classmethod
    def load(cls, note):
        return cls(note[0:2, :])

    def merge(self, other):
        return Sums(self.total + other)

    def rows(self):
        return stack_rows([self.total[0:1], self.total[1:2]], NOTE)


def insert(slot, place, side):
    low = slot & ((1 << place) - 1)
    return ((slot >> place) << (place + 1)) + (side << place) + low


def blocks_times(precond, value):
    width = 3 * FIBER_NODES
    fibers = precond.shape[1] // width
    nodes = fibers * FIBER_NODES
    results = []
    for fiber in range(fibers):
        parts = []
        for comp in range(3):
            first = comp * nodes + fiber * FIBER_NODES
            parts.append(value[first : first + FIBER_NODES])
        column = jnp.concatenate(parts, axis=0)
        blank = jnp.zeros_like(column)
        tall = [column if k == fiber else blank for k in range(fibers)]
        results.append(
            jnp.dot(
                precond,
                jnp.concatenate(tall, axis=0),
                precision=lax.Precision.HIGHEST,
                preferred_element_type=F32,
            )
        )
    parts = []
    for comp in range(3):
        for fiber in range(fibers):
            parts.append(results[fiber][comp * FIBER_NODES : (comp + 1) * FIBER_NODES])
    return jnp.concatenate(parts, axis=0)


def row_sum(first, second):
    return jnp.sum(first * second, axis=0, keepdims=True)


def first_body(right_hbm, precond_hbm, start_ref, sent_ref, right_ref, precond_ref, marks):
    height = start_ref.shape[0]
    loads = [
        pltpu.make_async_copy(right_hbm, right_ref, marks.at[0]),
        pltpu.make_async_copy(precond_hbm, precond_ref, marks.at[1]),
    ]
    for load in loads:
        load.start()
    for load in loads:
        load.wait()
    start = blocks_times(precond_ref[...], right_ref[...])
    start_ref[...] = start
    note = Scale(jnp.max(jnp.abs(start), axis=0, keepdims=True))
    sent_ref[0:height] = note.pack(start)
    sent_ref[height:] = note.packed


def couple_body(kind, places, near, sides_ref, tile_ref, got_ref, *refs):
    sends, keeps, note_ref, work_ref = refs[0:2], refs[2:4], refs[4], refs[5]
    sources = got_ref.shape[0]
    height = got_ref.shape[1] - EXTRA
    nodes = height // 3
    cases = got_ref.shape[2]
    half = cases // 2
    targets = tile_ref.shape[3] // nodes
    others = [kind.read(got_ref[k, height:]) for k in range(sources)]
    blocks = []
    for comp in range(3):
        for k in range(sources):
            block = got_ref[k, comp * nodes : (comp + 1) * nodes]
            if kind is Scale:
                block = block * others[k]
            blocks.append(block)
    value = jnp.concatenate(blocks, axis=0)
    terms = [value.astype(BF16)]
    if kind is Scale:
        note = Scale(functools.reduce(jnp.maximum, others))
        terms.append((value - terms[0].astype(F32)).astype(BF16))
    else:
        note = Sums(functools.reduce(jnp.add, others))
    note_ref[...] = note.rows()
    reach = targets // 2 * nodes
    base = (sides_ref[2] if near else 1 - sides_ref[2]) * reach
    for comp in range(3):
        left = tile_ref[:, comp, :, pl.ds(pl.multiple_of(base, reach), reach)]
        left = left.reshape(value.shape[0], reach)
        total = 0.0
        for term in terms:
            total = total + lax.dot_general(
                left, term, (((0,), (0,)), ((), ())), preferred_element_type=F32
            )
        work_ref[comp] = total
    slots = targets // 4
    for colour in range(2):
        first = colour * half
        columns = slice(first, first + half)
        side = sides_ref[colour]
        inner_note = type(note).load(note_ref[:, columns])
        send, kept = sends[colour], keeps[colour]
        for slot in range(slots):
            give = insert(slot, places[colour], 1 - side) * nodes
            keep = insert(slot, places[colour], side) * nodes
            for comp in range(3):
                row = slot * height + comp * nodes
                value = work_ref[comp, pl.ds(pl.multiple_of(give, nodes), nodes), columns]
                send[row : row + nodes] = inner_note.pack(value)
                value = work_ref[comp, pl.ds(pl.multiple_of(keep, nodes), nodes), columns]
                kept[row : row + nodes] = value
        send[slots * height :] = inner_note.packed


def merge_body(kind, places, height, sides_ref, note_ref, *refs):
    kept, got, outs, next_ref = refs[0:2], refs[2:4], refs[4:8], refs[8]
    half = kept[0].shape[1]
    slots = kept[0].shape[0] // height
    for colour in range(2):
        columns = slice(colour * half, (colour + 1) * half)
        side = sides_ref[colour]
        other = kind.read(got[colour][slots * height :])
        note = kind.load(note_ref[:, columns]).merge(other)
        next_ref[:, columns] = note.rows()
        for slot in range(slots // 2):
            rows = slice(slot * height, (slot + 1) * height)
            give = pl.ds(pl.multiple_of(insert(slot, places[colour], 1 - side) * height, height), height)
            keep = pl.ds(pl.multiple_of(insert(slot, places[colour], side) * height, height), height)
            outs[colour][rows] = note.pack(kept[colour][give] + kind.unpack(got[colour][give], other))
            outs[2 + colour][rows] = kept[colour][keep] + kind.unpack(got[colour][keep], other)
        outs[colour][slots // 2 * height :] = note.packed


def join_body(kind, note_ref, *refs):
    kept, got, sent_ref, next_ref = refs[0:2], refs[2:4], refs[4], refs[5]
    height, half = kept[0].shape
    for colour in range(2):
        columns = slice(colour * half, (colour + 1) * half)
        other = kind.read(got[colour][height:])
        note = kind.load(note_ref[:, columns]).merge(other)
        next_ref[:, columns] = note.rows()
        sent_ref[0:height, columns] = note.pack(
            kept[colour][...] + kind.unpack(got[colour][0:height], other)
        )
        sent_ref[height:, columns] = note.packed


def share_of(kind, kept, got, far_ref):
    height = kept[0].shape[0]
    parts = []
    for colour in range(2):
        other = kind.read(got[colour][height:])
        parts.append(kept[colour][...] + kind.unpack(got[colour][0:height], other))
    other = kind.read(far_ref[height:])
    return jnp.concatenate(parts, axis=1) + kind.unpack(far_ref[0:height], other), other


def second_body(*refs):
    kept, got, far_ref = refs[0:2], refs[2:4], refs[4]
    start_ref, precond_ref, work_ref, sent_ref = refs[5:]
    height = start_ref.shape[0]
    start = start_ref[...]
    share, _ = share_of(Scale, kept, got, far_ref)
    work = blocks_times(precond_ref[...], start + share)
    work_ref[...] = work
    note = Sums(jnp.concatenate([row_sum(start, start), row_sum(start, work)], axis=0))
    sent_ref[0:height] = note.pack(work)
    sent_ref[height:] = note.packed


def third_body(*refs):
    kept, got, far_ref = refs[0:2], refs[2:4], refs[4]
    note_ref, start_ref, work_ref, precond_ref, side_ref, gram_ref, next_ref = refs[5:]
    share, sums = share_of(Sums, kept, got, far_ref)
    note = Sums.load(note_ref[...]).merge(sums)
    next_ref[...] = note.rows()
    start = start_ref[...]
    work = work_ref[...]
    h_one_one = note.total[1:2] / (note.total[0:1] + TINY)
    other = blocks_times(precond_ref[...], work + share) - h_one_one * work
    side = work - h_one_one * start
    side_ref[...] = side
    pairs = [(side, side), (start, other), (side, other), (other, other)]
    rows = [row_sum(*pair) for pair in pairs]
    width = gram_ref.shape[1]
    count = rows[0].shape[1] // width
    parts = [row[:, k * width : (k + 1) * width] for row in rows for k in range(count)]
    gram_ref[...] = jnp.concatenate(parts, axis=0)


def last_body(flat_ref, note_ref, start_ref, side_ref, solution_ref, arnoldi_ref):
    total = jnp.sum(flat_ref[...], axis=0)
    count = total.shape[0] // 4
    gram = [
        jnp.concatenate([total[k * count + q : k * count + q + 1] for q in range(count)], axis=1)
        for k in range(4)
    ]
    side_side, start_other, side_other, other_other = gram
    square = note_ref[0:1, :] + TINY
    beta = jnp.sqrt(square)
    h_one_one = note_ref[1:2, :] / square
    h_two_one = jnp.sqrt(side_side / square + TINY)
    length = beta * h_two_one
    h_one_two = start_other / (beta * length)
    h_two_two = side_other / (length * length)
    loss_one = TINY / square
    loss_two = TINY / (h_two_one * h_two_one)
    one_two = h_one_one * loss_one / h_two_one
    rest = (
        other_other / (length * length)
        - h_one_two * h_one_two * (1.0 + loss_one)
        - h_two_two * h_two_two * (1.0 + loss_two)
        + 2.0 * h_one_two * h_two_two * one_two
    )
    h_three_two = jnp.sqrt(jnp.maximum(rest, 0.0) + TINY)
    y_one, y_two, estimate = least_squares(
        beta, h_one_one, h_two_one, h_one_two, h_two_two, h_three_two
    )
    solution_ref[...] = (y_one / beta) * start_ref[...] + (y_two / length) * side_ref[...]
    arnoldi_ref[0] = jnp.concatenate([h_one_one, h_one_two], axis=0)
    arnoldi_ref[1] = jnp.concatenate([h_two_one, h_two_two], axis=0)
    arnoldi_ref[2] = jnp.concatenate([estimate, h_three_two], axis=0)


def call(body, shapes, *args, scalars=0, outside=0, scratch=(), hold=True):
    spec = pl.BlockSpec(memory_space=pltpu.VMEM)
    far = pl.BlockSpec(memory_space=pltpu.HBM)
    small = pl.BlockSpec(memory_space=pltpu.SMEM)
    place = pltpu.VMEM if hold else pltpu.HBM
    held = [pltpu.with_memory_space_constraint(arg, place) for arg in args[scalars:]]
    inside = len(shapes) - outside
    return pl.pallas_call(
        body,
        out_shape=[pltpu.VMEM(shape, dtype) for shape, dtype in shapes[:inside]]
        + [jax.ShapeDtypeStruct(shape, dtype) for shape, dtype in shapes[inside:]],
        in_specs=[small] * scalars + [spec if hold else far] * len(held),
        out_specs=[spec] * len(shapes),
        scratch_shapes=list(scratch),
        compiler_params=pltpu.CompilerParams(vmem_limit_bytes=20 * 1024 * 1024),
    )(*args[:scalars], *held)


def travel(array, kind, move):
    if kind is Scale:
        return move(array.astype(jnp.float16)).astype(F32)
    return move(array)


def build(bits):
    lower = bits[1:]
    orders = (list(reversed(lower)), list(lower))

    def local(mobility, right_side, precond):
        row_count = mobility.shape[5]
        sources = mobility.shape[2]
        node_dev = mobility.shape[4]
        cases = right_side.shape[2]
        height = 3 * node_dev
        half = cases // 2
        tile = mobility.reshape(3, 3, sources * node_dev, row_count)
        right = right_side.reshape(height, cases)

        def sides(names):
            return jnp.stack([lax.axis_index(name).astype(jnp.int32) for name in names])

        def gather(sent, kind):
            return travel(sent, kind, lambda a: lax.all_gather(a, ("row", "core")))

        def cast(array, kind):
            return array.astype(jnp.float16) if kind is Scale else array

        def widen(array, kind):
            return array.astype(F32) if kind is Scale else array

        def swap(arrays, names, kind):
            moved = [lax.ppermute(cast(a, kind), name, SWAP) for a, name in zip(arrays, names)]
            return [widen(a, kind) for a in moved]

        def exchange(got, kind):
            left = [list(lower), list(lower)]
            note = ((NOTE, cases), F32)
            slots = row_count // node_dev // 2

            def take(step):
                names = [orders[0][step], orders[1][step]]
                places = [len(left[k]) - 1 - left[k].index(names[k]) for k in range(2)]
                for k in range(2):
                    left[k].remove(names[k])
                return names, places

            def shapes(count):
                tall = count * height
                return [((tall + EXTRA, half), kind.sent)], [((tall, half), F32)]

            names, places = take(0)
            slots = slots // 2
            sent, kept = shapes(slots)
            pair = []
            for near in range(2):
                outs = call(
                    functools.partial(couple_body, kind, places, near),
                    sent * 2 + kept * 2 + [note],
                    sides(names + [bits[0]]),
                    tile,
                    got,
                    scalars=1,
                    scratch=[pltpu.VMEM((3, row_count // 2, cases), F32)],
                )
                pair.append([outs[0:2], outs[2:4], outs[4]])
            far, near = pair
            plan = [(names, None)]
            for step in range(1, len(lower)):
                plan.append(take(step))

            def reduce(state, tie):
                count = slots
                sends, kept, notes = state
                arrived = swap(sends, plan[0][0], kind)
                if tie is not None:
                    arrived = list(lax.optimization_barrier(tuple(arrived) + (near[2],))[:2])
                for names, places in plan[1:]:
                    count = count // 2
                    sent, keep = shapes(count)
                    outs = call(
                        functools.partial(merge_body, kind, places, height),
                        sent * 2 + keep * 2 + [note],
                        sides(names),
                        notes,
                        *kept,
                        *arrived,
                        scalars=1,
                    )
                    if tie is not None:
                        tie.append(outs[4])
                    kept, notes = outs[2:4], outs[4]
                    arrived = swap(outs[0:2], names, kind)
                return kept, arrived, notes

            ties = []
            kept, arrived, notes = reduce(far, ties)
            sent, notes = call(
                functools.partial(join_body, kind),
                [((height + EXTRA, cases), kind.sent), note],
                notes,
                *kept,
                *arrived,
            )
            if ties:
                tied = lax.optimization_barrier(tuple(near[0]) + (ties[0],))
                near[0] = list(tied[:2])
            (crossed,) = swap([sent], [bits[0]], kind)
            kept, arrived, _ = reduce(near, None)
            return list(kept) + list(arrived) + [crossed], notes

        full = ((height, cases), F32)
        packed = ((height + EXTRA, cases), F32)
        start, sent = call(
            first_body,
            [full, packed],
            right,
            precond,
            hold=False,
            scratch=[
                pltpu.VMEM(right.shape, F32),
                pltpu.VMEM(precond.shape, F32),
                pltpu.SemaphoreType.DMA((2,)),
            ],
        )
        shares, _ = exchange(gather(sent, Scale), Scale)
        packed = ((height + EXTRA, cases), BF16)
        work, sent = call(second_body, [full, packed], *shares, start, precond)
        shares, notes = exchange(gather(sent, Sums), Sums)
        side, flat, notes = call(
            third_body,
            [full, ((4 * cases // 128, 128), F32), ((NOTE, cases), F32)],
            *shares,
            notes,
            start,
            work,
            precond,
        )
        flat = flat + lax.ppermute(flat, "core", SWAP)
        members = sources // 2 * 2 ** len(bits)
        flat = lax.all_to_all(
            jnp.broadcast_to(flat, (members,) + flat.shape), ("row",) + tuple(bits), 0, 0
        )
        answer, arnoldi = call(last_body, [full, ((3, 2, cases), F32)], flat, notes, start, side, outside=2)
        return answer.reshape(3, node_dev, cases), arnoldi

    return local


def solution(mesh):
    count_tgt, count_src = mesh.shape["tgt"], mesh.shape["src"]
    depth = count_src.bit_length() - 1
    bits = ["bit%d" % k for k in reversed(range(depth))]
    tgt = ("row", "core")
    src = tuple(bits)
    grid = mesh.devices.reshape((count_tgt // 2, 2) + (2,) * depth)
    placed = (
        P(None, None, None, src, None, tgt),
        P(None, tgt + src, None),
        P(None, tgt + src),
    )
    return jax.shard_map(
        build(bits),
        mesh=Mesh(grid, tgt + src),
        in_specs=placed,
        out_specs=(P(None, tgt + src, None), P()),
        check_vma=False,
    )
```

```python
import functools

import jax
import jax.numpy as jnp
from jax import lax
from jax.experimental import pallas as pl
from jax.experimental.pallas import tpu as pltpu
from jax.sharding import Mesh, PartitionSpec as P

FIBER_NODES = 32
PIECES = 3
EXTRA = 8
NOTE = 8
SWAP = [(0, 1), (1, 0)]
TINY = 1e-06
F32 = jnp.float32
BF16 = jnp.bfloat16


def least_squares(beta, h_one_one, h_two_one, h_one_two, h_two_two, h_three_two):
    rho_one = jnp.sqrt(h_one_one * h_one_one + h_two_one * h_two_one)
    cos_one = h_one_one / rho_one
    sin_one = h_two_one / rho_one
    g_one = cos_one * beta
    g_two = -sin_one * beta
    top = cos_one * h_one_two + sin_one * h_two_two
    low = cos_one * h_two_two - sin_one * h_one_two
    rho_two = jnp.sqrt(low * low + h_three_two * h_three_two)
    cos_two = low / rho_two
    sin_two = h_three_two / rho_two
    y_two = cos_two * g_two / rho_two
    y_one = (g_one - top * y_two) / rho_one
    return (y_one, y_two, jnp.abs(sin_two * g_two))


def stack_rows(rows, count):
    blank = jnp.zeros_like(rows[0])
    return jnp.concatenate(list(rows) + [blank] * (count - len(rows)), axis=0)


class Scale:
    sent = F32

    def __init__(self, size):
        factors = []
        scale = jnp.ones_like(size)
        rest = size
        for _ in range(PIECES):
            factor = jnp.clip(rest, 2.0**-13, 2.0**15).astype(BF16).astype(F32)
            factors.append(factor)
            scale = scale * factor
            rest = rest / factor
        self.scale = scale
        self.inverse = 1.0 / scale
        self.packed = stack_rows(factors, EXTRA)

    def pack(self, body):
        return body * self.inverse

    @staticmethod
    def read(rows):
        return rows[0:1] * rows[1:2] * rows[2:3]

    @staticmethod
    def unpack(body, other):
        return body * other

    @classmethod
    def load(cls, note):
        return cls(note[0:1, :])

    def merge(self, other):
        return Scale(jnp.maximum(self.scale, other))

    def rows(self):
        return stack_rows([self.scale], NOTE)


class Sums:
    sent = BF16

    def __init__(self, total):
        pieces = []
        rest = total
        for _ in range(PIECES):
            piece = rest.astype(BF16).astype(F32)
            pieces.append(piece)
            rest = rest - piece
        self.total = total
        rows = [piece[k : k + 1] for piece in pieces for k in range(2)]
        self.packed = stack_rows(rows, EXTRA).astype(BF16)

    def pack(self, body):
        return body.astype(BF16)

    @staticmethod
    def read(rows):
        wide = rows.astype(F32)
        return wide[0:2] + wide[2:4] + wide[4:6]

    @staticmethod
    def unpack(body, other):
        return body.astype(F32)

    @classmethod
    def load(cls, note):
        return cls(note[0:2, :])

    def merge(self, other):
        return Sums(self.total + other)

    def rows(self):
        return stack_rows([self.total[0:1], self.total[1:2]], NOTE)


def insert(slot, place, side):
    low = slot & ((1 << place) - 1)
    return ((slot >> place) << (place + 1)) + (side << place) + low


def blocks_times(precond, value):
    width = 3 * FIBER_NODES
    fibers = precond.shape[1] // width
    nodes = fibers * FIBER_NODES
    results = []
    for fiber in range(fibers):
        parts = []
        for comp in range(3):
            first = comp * nodes + fiber * FIBER_NODES
            parts.append(value[first : first + FIBER_NODES])
        column = jnp.concatenate(parts, axis=0)
        blank = jnp.zeros_like(column)
        tall = [column if k == fiber else blank for k in range(fibers)]
        results.append(
            jnp.dot(
                precond,
                jnp.concatenate(tall, axis=0),
                precision=lax.Precision.HIGHEST,
                preferred_element_type=F32,
            )
        )
    parts = []
    for comp in range(3):
        for fiber in range(fibers):
            parts.append(results[fiber][comp * FIBER_NODES : (comp + 1) * FIBER_NODES])
    return jnp.concatenate(parts, axis=0)


def row_sum(first, second):
    return jnp.sum(first * second, axis=0, keepdims=True)


def first_body(right_hbm, precond_hbm, start_ref, sent_ref, right_ref, precond_ref, marks):
    height = start_ref.shape[0]
    loads = [
        pltpu.make_async_copy(right_hbm, right_ref, marks.at[0]),
        pltpu.make_async_copy(precond_hbm, precond_ref, marks.at[1]),
    ]
    for load in loads:
        load.start()
    for load in loads:
        load.wait()
    start = blocks_times(precond_ref[...], right_ref[...])
    start_ref[...] = start
    note = Scale(jnp.max(jnp.abs(start), axis=0, keepdims=True))
    sent_ref[0:height] = note.pack(start)
    sent_ref[height:] = note.packed


def couple_body(kind, places, near, sides_ref, tile_ref, got_ref, *refs):
    sends, keeps, note_ref, work_ref = refs[0:2], refs[2:4], refs[4], refs[5]
    sources = got_ref.shape[0]
    height = got_ref.shape[1] - EXTRA
    nodes = height // 3
    cases = got_ref.shape[2]
    half = cases // 2
    targets = tile_ref.shape[3] // nodes
    others = [kind.read(got_ref[k, height:]) for k in range(sources)]
    blocks = []
    for comp in range(3):
        for k in range(sources):
            block = got_ref[k, comp * nodes : (comp + 1) * nodes]
            if kind is Scale:
                block = block * others[k]
            blocks.append(block)
    value = jnp.concatenate(blocks, axis=0)
    terms = [value.astype(BF16)]
    if kind is Scale:
        note = Scale(functools.reduce(jnp.maximum, others))
        terms.append((value - terms[0].astype(F32)).astype(BF16))
    else:
        note = Sums(functools.reduce(jnp.add, others))
    note_ref[...] = note.rows()
    reach = targets // 2 * nodes
    base = (sides_ref[2] if near else 1 - sides_ref[2]) * reach
    for comp in range(3):
        left = tile_ref[:, comp, :, pl.ds(pl.multiple_of(base, reach), reach)]
        left = left.reshape(value.shape[0], reach)
        total = 0.0
        for term in terms:
            total = total + lax.dot_general(
                left, term, (((0,), (0,)), ((), ())), preferred_element_type=F32
            )
        work_ref[comp] = total
    slots = targets // 4
    for colour in range(2):
        first = colour * half
        columns = slice(first, first + half)
        side = sides_ref[colour]
        inner_note = type(note).load(note_ref[:, columns])
        send, kept = sends[colour], keeps[colour]
        for slot in range(slots):
            give = insert(slot, places[colour], 1 - side) * nodes
            keep = insert(slot, places[colour], side) * nodes
            for comp in range(3):
                row = slot * height + comp * nodes
                value = work_ref[comp, pl.ds(pl.multiple_of(give, nodes), nodes), columns]
                send[row : row + nodes] = inner_note.pack(value)
                value = work_ref[comp, pl.ds(pl.multiple_of(keep, nodes), nodes), columns]
                kept[row : row + nodes] = value
        send[slots * height :] = inner_note.packed


def merge_body(kind, places, height, sides_ref, note_ref, *refs):
    kept, got, outs, next_ref = refs[0:2], refs[2:4], refs[4:8], refs[8]
    half = kept[0].shape[1]
    slots = kept[0].shape[0] // height
    for colour in range(2):
        columns = slice(colour * half, (colour + 1) * half)
        side = sides_ref[colour]
        other = kind.read(got[colour][slots * height :])
        note = kind.load(note_ref[:, columns]).merge(other)
        next_ref[:, columns] = note.rows()
        for slot in range(slots // 2):
            rows = slice(slot * height, (slot + 1) * height)
            give = pl.ds(pl.multiple_of(insert(slot, places[colour], 1 - side) * height, height), height)
            keep = pl.ds(pl.multiple_of(insert(slot, places[colour], side) * height, height), height)
            outs[colour][rows] = note.pack(kept[colour][give] + kind.unpack(got[colour][give], other))
            outs[2 + colour][rows] = kept[colour][keep] + kind.unpack(got[colour][keep], other)
        outs[colour][slots // 2 * height :] = note.packed


def join_body(kind, note_ref, *refs):
    kept, got, sent_ref, next_ref = refs[0:2], refs[2:4], refs[4], refs[5]
    height, half = kept[0].shape
    for colour in range(2):
        columns = slice(colour * half, (colour + 1) * half)
        other = kind.read(got[colour][height:])
        note = kind.load(note_ref[:, columns]).merge(other)
        next_ref[:, columns] = note.rows()
        sent_ref[0:height, columns] = note.pack(
            kept[colour][...] + kind.unpack(got[colour][0:height], other)
        )
        sent_ref[height:, columns] = note.packed


def share_of(kind, kept, got, far_ref):
    height = kept[0].shape[0]
    parts = []
    for colour in range(2):
        other = kind.read(got[colour][height:])
        parts.append(kept[colour][...] + kind.unpack(got[colour][0:height], other))
    other = kind.read(far_ref[height:])
    return jnp.concatenate(parts, axis=1) + kind.unpack(far_ref[0:height], other), other


def second_body(*refs):
    kept, got, far_ref = refs[0:2], refs[2:4], refs[4]
    start_ref, precond_ref, work_ref, sent_ref = refs[5:]
    height = start_ref.shape[0]
    start = start_ref[...]
    share, _ = share_of(Scale, kept, got, far_ref)
    work = blocks_times(precond_ref[...], start + share)
    work_ref[...] = work
    note = Sums(jnp.concatenate([row_sum(start, start), row_sum(start, work)], axis=0))
    sent_ref[0:height] = note.pack(work)
    sent_ref[height:] = note.packed


def third_body(*refs):
    kept, got, far_ref = refs[0:2], refs[2:4], refs[4]
    note_ref, start_ref, work_ref, precond_ref, side_ref, gram_ref, next_ref = refs[5:]
    share, sums = share_of(Sums, kept, got, far_ref)
    note = Sums.load(note_ref[...]).merge(sums)
    next_ref[...] = note.rows()
    start = start_ref[...]
    work = work_ref[...]
    h_one_one = note.total[1:2] / (note.total[0:1] + TINY)
    other = blocks_times(precond_ref[...], work + share) - h_one_one * work
    side = work - h_one_one * start
    side_ref[...] = side
    pairs = [(side, side), (start, other), (side, other), (other, other)]
    rows = [row_sum(*pair) for pair in pairs]
    width = gram_ref.shape[1]
    count = rows[0].shape[1] // width
    parts = [row[:, k * width : (k + 1) * width] for row in rows for k in range(count)]
    gram_ref[...] = jnp.concatenate(parts, axis=0)


def last_body(flat_ref, note_ref, start_ref, side_ref, solution_ref, arnoldi_ref):
    total = jnp.sum(flat_ref[...], axis=0)
    count = total.shape[0] // 4
    gram = [
        jnp.concatenate([total[k * count + q : k * count + q + 1] for q in range(count)], axis=1)
        for k in range(4)
    ]
    side_side, start_other, side_other, other_other = gram
    square = note_ref[0:1, :] + TINY
    beta = jnp.sqrt(square)
    h_one_one = note_ref[1:2, :] / square
    h_two_one = jnp.sqrt(side_side / square + TINY)
    length = beta * h_two_one
    h_one_two = start_other / (beta * length)
    h_two_two = side_other / (length * length)
    loss_one = TINY / square
    loss_two = TINY / (h_two_one * h_two_one)
    one_two = h_one_one * loss_one / h_two_one
    rest = (
        other_other / (length * length)
        - h_one_two * h_one_two * (1.0 + loss_one)
        - h_two_two * h_two_two * (1.0 + loss_two)
        + 2.0 * h_one_two * h_two_two * one_two
    )
    h_three_two = jnp.sqrt(jnp.maximum(rest, 0.0) + TINY)
    y_one, y_two, estimate = least_squares(
        beta, h_one_one, h_two_one, h_one_two, h_two_two, h_three_two
    )
    solution_ref[...] = (y_one / beta) * start_ref[...] + (y_two / length) * side_ref[...]
    arnoldi_ref[0] = jnp.concatenate([h_one_one, h_one_two], axis=0)
    arnoldi_ref[1] = jnp.concatenate([h_two_one, h_two_two], axis=0)
    arnoldi_ref[2] = jnp.concatenate([estimate, h_three_two], axis=0)


def call(body, shapes, *args, scalars=0, outside=0, scratch=(), hold=True):
    spec = pl.BlockSpec(memory_space=pltpu.VMEM)
    far = pl.BlockSpec(memory_space=pltpu.HBM)
    small = pl.BlockSpec(memory_space=pltpu.SMEM)
    place = pltpu.VMEM if hold else pltpu.HBM
    held = [pltpu.with_memory_space_constraint(arg, place) for arg in args[scalars:]]
    inside = len(shapes) - outside
    return pl.pallas_call(
        body,
        out_shape=[pltpu.VMEM(shape, dtype) for shape, dtype in shapes[:inside]]
        + [jax.ShapeDtypeStruct(shape, dtype) for shape, dtype in shapes[inside:]],
        in_specs=[small] * scalars + [spec if hold else far] * len(held),
        out_specs=[spec] * len(shapes),
        scratch_shapes=list(scratch),
        compiler_params=pltpu.CompilerParams(vmem_limit_bytes=20 * 1024 * 1024),
    )(*args[:scalars], *held)


def travel(array, kind, move):
    if kind is Scale:
        return move(array.astype(jnp.float16)).astype(F32)
    return move(array)


def build(bits):
    lower = bits[1:]
    orders = (list(lower), list(reversed(lower)))

    def local(mobility, right_side, precond):
        row_count = mobility.shape[5]
        sources = mobility.shape[2]
        node_dev = mobility.shape[4]
        cases = right_side.shape[2]
        height = 3 * node_dev
        half = cases // 2
        tile = mobility.reshape(3, 3, sources * node_dev, row_count)
        right = right_side.reshape(height, cases)

        def sides(names):
            return jnp.stack([lax.axis_index(name).astype(jnp.int32) for name in names])

        def gather(sent, kind):
            return travel(sent, kind, lambda a: lax.all_gather(a, ("row", "core")))

        def cast(array, kind):
            return array.astype(jnp.float16) if kind is Scale else array

        def widen(array, kind):
            return array.astype(F32) if kind is Scale else array

        def swap(arrays, names, kind):
            moved = [lax.ppermute(cast(a, kind), name, SWAP) for a, name in zip(arrays, names)]
            return [widen(a, kind) for a in moved]

        def exchange(got, kind):
            left = [list(lower), list(lower)]
            note = ((NOTE, cases), F32)
            slots = row_count // node_dev // 2

            def take(step):
                names = [orders[0][step], orders[1][step]]
                places = [len(left[k]) - 1 - left[k].index(names[k]) for k in range(2)]
                for k in range(2):
                    left[k].remove(names[k])
                return names, places

            def shapes(count):
                tall = count * height
                return [((tall + EXTRA, half), kind.sent)], [((tall, half), F32)]

            names, places = take(0)
            slots = slots // 2
            sent, kept = shapes(slots)
            pair = []
            for near in range(2):
                outs = call(
                    functools.partial(couple_body, kind, places, near),
                    sent * 2 + kept * 2 + [note],
                    sides(names + [bits[0]]),
                    tile,
                    got,
                    scalars=1,
                    scratch=[pltpu.VMEM((3, row_count // 2, cases), F32)],
                )
                pair.append([outs[0:2], outs[2:4], outs[4]])
            far, near = pair
            plan = [(names, None)]
            for step in range(1, len(lower)):
                plan.append(take(step))

            def reduce(state, tie):
                count = slots
                sends, kept, notes = state
                arrived = swap(sends, plan[0][0], kind)
                if tie is not None:
                    arrived = list(lax.optimization_barrier(tuple(arrived) + (near[2],))[:2])
                for names, places in plan[1:]:
                    count = count // 2
                    sent, keep = shapes(count)
                    outs = call(
                        functools.partial(merge_body, kind, places, height),
                        sent * 2 + keep * 2 + [note],
                        sides(names),
                        notes,
                        *kept,
                        *arrived,
                        scalars=1,
                    )
                    if tie is not None:
                        tie.append(outs[4])
                    kept, notes = outs[2:4], outs[4]
                    arrived = swap(outs[0:2], names, kind)
                return kept, arrived, notes

            ties = []
            kept, arrived, notes = reduce(far, ties)
            sent, notes = call(
                functools.partial(join_body, kind),
                [((height + EXTRA, cases), kind.sent), note],
                notes,
                *kept,
                *arrived,
            )
            if ties:
                tied = lax.optimization_barrier(tuple(near[0]) + (ties[0],))
                near[0] = list(tied[:2])
            (crossed,) = swap([sent], [bits[0]], kind)
            kept, arrived, _ = reduce(near, None)
            return list(kept) + list(arrived) + [crossed], notes

        full = ((height, cases), F32)
        packed = ((height + EXTRA, cases), F32)
        start, sent = call(
            first_body,
            [full, packed],
            right,
            precond,
            hold=False,
            scratch=[
                pltpu.VMEM(right.shape, F32),
                pltpu.VMEM(precond.shape, F32),
                pltpu.SemaphoreType.DMA((2,)),
            ],
        )
        shares, _ = exchange(gather(sent, Scale), Scale)
        packed = ((height + EXTRA, cases), BF16)
        work, sent = call(second_body, [full, packed], *shares, start, precond)
        shares, notes = exchange(gather(sent, Sums), Sums)
        side, flat, notes = call(
            third_body,
            [full, ((4 * cases // 128, 128), F32), ((NOTE, cases), F32)],
            *shares,
            notes,
            start,
            work,
            precond,
        )
        flat = flat + lax.ppermute(flat, "core", SWAP)
        members = sources // 2 * 2 ** len(bits)
        flat = lax.all_to_all(
            jnp.broadcast_to(flat, (members,) + flat.shape), ("row",) + tuple(bits), 0, 0
        )
        answer, arnoldi = call(last_body, [full, ((3, 2, cases), F32)], flat, notes, start, side, outside=2)
        return answer.reshape(3, node_dev, cases), arnoldi

    return local


def solution(mesh):
    count_tgt, count_src = mesh.shape["tgt"], mesh.shape["src"]
    depth = count_src.bit_length() - 1
    bits = ["bit%d" % k for k in reversed(range(depth))]
    tgt = ("row", "core")
    src = tuple(bits)
    grid = mesh.devices.reshape((count_tgt // 2, 2) + (2,) * depth)
    placed = (
        P(None, None, None, src, None, tgt),
        P(None, tgt + src, None),
        P(None, tgt + src),
    )
    return jax.shard_map(
        build(bits),
        mesh=Mesh(grid, tgt + src),
        in_specs=placed,
        out_specs=(P(None, tgt + src, None), P()),
        check_vma=False,
    )
```
